128 devices in a mesh: gx: 16 (over z, x), yz: 8 (over y, core).
Axes of the slice: x: 4, y: 4, z: 4, core: 2. Of those that a mesh axis runs over, the one named last changes fastest.
Arguments:
- populations: float32 [19, 128, 64, 128], P(None, 'gx', 'yz'), may hold values from 0.02 to 0.1
- cell_grain: int32 [128, 64, 128], P('gx', 'yz'), may hold values from -1 to 1023, as said below
- near_rows: int32 [128, 1024], P(('gx', 'yz')), may hold values from -1 to 511, as said below
- contact_pairs: int32 [2, 131072], P(None, ('gx', 'yz')), may hold values from 0 to 1023, as said below
- grain_position: float32 [3, 65536], P(None, ('gx', 'yz')), may hold values from 0 to 6
- grain_velocity: float32 [3, 65536], P(None, ('gx', 'yz')), may hold values from -0.1 to 0.1
- grain_radius: float32 [65536], P(('gx', 'yz')), may hold values from 0.8 to 1.6
- grain_mass: float32 [65536], P(('gx', 'yz')), may hold values from 2 to 20
Outputs:
- populations_next: float32 [19, 128, 64, 128], P(None, 'gx', 'yz')
- velocity_next: float32 [3, 65536], P(None, ('gx', 'yz'))
- position_next: float32 [3, 65536], P(None, ('gx', 'yz'))
The draws below stay inside these ranges and needn't reach their ends.
Inputs may be any that keep to these rules, and one draw needn't show every extreme that they name: `near_rows`: entry o * 8 + s of device d's row names a row of device o's grains or is -1; in each block of 8 entries the live ones come first, are distinct, and number 1 to 8; every device has one block with all 8 live. `cell_grain`: A solid cell names a live entry of the list of the device whose brick holds it; the share of solid cells differs from brick to brick. `contact_pairs`: column p belongs to device p // 1024: its first row is a row of that device's grains, its second a live entry of that device's list.
All inputs are finite; a program needn't handle non-finite values.
Results may differ from the reference program's by a relative error of at most 0.0003.
Values sent between devices are 32-bit elements; how exact they have to be, the bound alone decides.
No kernel may reach another device: no remote copies, remote signals or barrier semaphores. Data moves between devices by JAX's collectives and lax.ppermute only.
A program may use at most 64 MiB of HBM per device.

```python
import math
import jax
import jax.numpy as jnp
import numpy as np
from jax import lax

CX = 8
CY = 8
CZ = 128
GR_DEV = 512
NEAR = 1024
PAIRS_DEV = 1024
SLOT = 8
NX = 128
NY = 64
GRAINS = 65536
PAIRS = 131072
N_YZ = 8
DEVICES = 128


def grain_layout(key):
    base = jax.random.fold_in(key, 7)
    key_count, key_full, key_rows = jax.random.split(base, 3)
    counts = jax.random.randint(key_count, (DEVICES, DEVICES), 1, SLOT + 1)
    full = jax.random.randint(key_full, (DEVICES,), 0, DEVICES)
    counts = jnp.where(jnp.arange(DEVICES)[None, :] == full[:, None], SLOT, counts)
    return (counts.astype(jnp.int32), key_rows)


def live_entry(key, device, counts):
    key_owner, key_slot = jax.random.split(key)
    owner = jax.random.randint(key_owner, device.shape, 0, DEVICES)
    slot = jax.random.randint(key_slot, device.shape, 0, counts[device, owner])
    return (owner * SLOT + slot).astype(jnp.int32)


def draw_near_rows(key, part):
    counts, key_rows = grain_layout(key)
    scores = jax.random.randint(key_rows, (DEVICES, DEVICES, GR_DEV), 0, 2 ** 30 // GR_DEV)
    scores = scores * GR_DEV + jnp.arange(GR_DEV, dtype=jnp.int32)
    picked = lax.top_k(scores, SLOT)[1]
    slots = jnp.arange(SLOT, dtype=jnp.int32)
    rows = jnp.where(slots[None, None, :] < counts[:, :, None], picked, -1)
    return rows.reshape(DEVICES, NEAR).astype(jnp.int32)


def draw_cell_grain(key, part):
    counts, key_rows = grain_layout(key)
    base = jax.random.fold_in(key, 19)
    key_share, key_solid, key_entry = jax.random.split(base, 3)
    device = (jnp.arange(NX, dtype=jnp.int32) // CX)[:, None, None] * N_YZ + (jnp.arange(NY, dtype=jnp.int32) // CY)[None, :, None]
    device = jnp.broadcast_to(device, (NX, NY, CZ))
    share = jax.random.randint(key_share, (DEVICES,), 10, 61)
    solid = jax.random.randint(key_solid, (NX, NY, CZ), 0, 100) < share[device]
    entry = live_entry(key_entry, device, counts)
    return jnp.where(solid, entry, -1).astype(jnp.int32)


def draw_contact_pairs(key, part):
    counts, key_rows = grain_layout(key)
    base = jax.random.fold_in(key, 31)
    key_first, key_second = jax.random.split(base)
    device = jnp.arange(PAIRS, dtype=jnp.int32) // PAIRS_DEV
    first = jax.random.randint(key_first, (PAIRS,), 0, GR_DEV)
    second = live_entry(key_second, device, counts)
    return jnp.stack([first.astype(jnp.int32), second]).astype(jnp.int32)


def levels(stream_key, extent, cuts, low, top_value):
    gain = 1.0
    for axis_at, blocks in cuts:
        draws = jax.random.uniform(jax.random.fold_in(jax.random.fold_in(stream_key, 6), axis_at), (blocks,), jnp.float32, low / len(cuts), top_value / len(cuts))
        gain = gain * jnp.repeat(jnp.exp(draws), extent[axis_at] // blocks).reshape((-1,) + (1,) * (len(extent) - 1 - axis_at))
    return gain


def setup_inputs(seed: int = 0) -> dict:
    keys = jax.random.split(jax.random.key(seed), 9)
    populations = jnp.clip(0.02 + 0.08 * jax.random.uniform(keys[0], (19, NX, NY, CZ), jnp.float32) ** levels(keys[0], (19, NX, NY, CZ), ((1, 16), (2, 8)), -0.2, 0.2), 0.02, 0.1)
    cell_grain = draw_cell_grain(jax.random.fold_in(keys[8], 71), 0)
    near_rows = draw_near_rows(jax.random.fold_in(keys[8], 71), 0)
    contact_pairs = draw_contact_pairs(jax.random.fold_in(keys[8], 71), 0)
    grain_position = jnp.clip(6.0 * jax.random.uniform(keys[4], (3, GRAINS), jnp.float32) ** levels(keys[4], (3, GRAINS), ((1, 128),), -0.2, 0.2), 0.0, 6.0)
    grain_velocity = jnp.clip(jax.random.uniform(keys[5], (3, GRAINS), jnp.float32, -0.1, 0.1) * levels(keys[5], (3, GRAINS), ((1, 128),), -0.4, 0.0), -0.1, 0.1)
    grain_radius = jnp.clip(0.8 + 0.8 * jax.random.uniform(keys[6], (GRAINS,), jnp.float32) ** levels(keys[6], (GRAINS,), ((0, 128),), -0.2, 0.2), 0.8, 1.6)
    grain_mass = jnp.clip(jnp.exp(math.log(20.0) - 2.3025851 * jax.random.uniform(keys[7], (GRAINS,), jnp.float32) ** levels(keys[7], (GRAINS,), ((0, 128),), -0.2, 0.2)), 2.0, 20.0)
    return dict(populations=populations, cell_grain=cell_grain, near_rows=near_rows, contact_pairs=contact_pairs, grain_position=grain_position, grain_velocity=grain_velocity, grain_radius=grain_radius, grain_mass=grain_mass)


lattice_dirs = ((0, 0, 0), (1, 0, 0), (-1, 0, 0), (0, 1, 0), (0, -1, 0), (0, 0, 1), (0, 0, -1), (1, 1, 0), (-1, -1, 0), (1, -1, 0), (-1, 1, 0), (1, 0, 1), (-1, 0, -1), (1, 0, -1), (-1, 0, 1), (0, 1, 1), (0, -1, -1), (0, 1, -1), (0, -1, 1))
lattice_weights = (1.0 / 3.0,) + (1.0 / 18.0,) * 6 + (1.0 / 36.0,) * 12
opposite = (0, 2, 1, 4, 3, 6, 5, 8, 7, 10, 9, 12, 11, 14, 13, 16, 15, 18, 17)
relax_rate = 1.25
stiffness = 0.5
damping = 0.5

def project(direction, parts):
    total = None
    for compo in range(3):
        factor = lattice_dirs[direction][compo]
        if factor != 0:
            term = factor * parts[compo]
            total = term if total is None else total + term
    return total

def collide(populations):
    density = lax.optimization_barrier(jnp.sum(populations, axis=0))
    speeds = []
    for compo in range(3):
        moment = jnp.zeros_like(density)
        for direction in range(19):
            factor = lattice_dirs[direction][compo]
            if factor != 0:
                moment = moment + factor * populations[direction]
        speeds.append(moment / density)
    square = speeds[0] * speeds[0] + speeds[1] * speeds[1] + speeds[2] * speeds[2]
    result = []
    for direction in range(19):
        if direction == 0:
            equil = lattice_weights[0] * density * (1.0 - 1.5 * square)
        else:
            along = project(direction, speeds)
            equil = lattice_weights[direction] * density * (1.0 + 3.0 * along + 4.5 * along * along - 1.5 * square)
        result.append(populations[direction] + relax_rate * (equil - populations[direction]))
    return jnp.stack(result)

def stream_force(populations, fluid, pick):
    here = pick(list(range(24)), 0, 0, 0)
    fresh = [here[0]]
    force = [jnp.zeros_like(here[0]) for compo in range(3)]
    for direction in range(1, 19):
        shift_x, shift_y, shift_z = lattice_dirs[direction]
        back = opposite[direction]
        weight = lattice_weights[direction]
        source = pick([direction, 19, 20, 21, 22], shift_x, shift_y, shift_z)
        bounce = here[back] + 6.0 * weight * here[23] * project(direction, source[1:4])
        fresh.append(source[4] * source[0] + (1.0 - source[4]) * bounce)
        target = pick([back, 22, 23], -shift_x, -shift_y, -shift_z)
        link = target[1] * (2.0 * target[0] + 6.0 * weight * target[2] * project(direction, here[19:22])) * (1.0 - here[22])
        for compo in range(3):
            factor = lattice_dirs[direction][compo]
            if factor != 0:
                force[compo] = force[compo] - factor * link
    read = jnp.where(fluid[None], jnp.stack(fresh), populations)
    return (read, jnp.stack(force))

def contact_force(pos_a, vel_a, rad_a, pos_b, vel_b, rad_b):
    offset = pos_a - pos_b
    length = jnp.sqrt(lax.optimization_barrier(jnp.sum(offset * offset, axis=0)))
    normal = offset / jnp.maximum(length, 1.0)
    intersection = jnp.maximum(rad_a + rad_b - length, 0.0)
    closing = lax.optimization_barrier(jnp.sum((vel_a - vel_b) * normal, axis=0))
    return (stiffness * intersection - damping * intersection * closing) * normal

def reference(populations, cell_grain, near_rows, contact_pairs, grain_position, grain_velocity, grain_radius, grain_mass):
    slot_owner = jnp.arange(NEAR, dtype=jnp.int32) // SLOT
    near_grain = slot_owner[None, :] * GR_DEV + jnp.maximum(near_rows, 0)
    brick = (jnp.arange(NX, dtype=jnp.int32) // CX)[:, None, None] * N_YZ + (jnp.arange(NY, dtype=jnp.int32) // CY)[None, :, None]
    solid = cell_grain >= 0
    grain_cell = near_grain[brick, jnp.maximum(cell_grain, 0)]
    wall = grain_velocity[:, grain_cell] * solid.astype(jnp.float32)[None]
    post = collide(populations)
    table = jnp.concatenate([post, wall, (~solid).astype(jnp.float32)[None], lax.optimization_barrier(jnp.sum(post, axis=0))[None]], 0)

    def pick(channels, shift_x, shift_y, shift_z):
        return jnp.roll(table[np.array(channels)], (shift_x, shift_y, shift_z), axis=(1, 2, 3))
    read, cell_force = stream_force(populations, ~solid, pick)
    flat_ids = jnp.where(solid, grain_cell, GRAINS).reshape(-1).astype(jnp.int32)
    fluid_force = jax.ops.segment_sum(cell_force.reshape(3, -1).T, flat_ids, GRAINS + 1)[:GRAINS].T
    pair_dev = jnp.arange(PAIRS, dtype=jnp.int32) // PAIRS_DEV
    first = pair_dev * GR_DEV + contact_pairs[0]
    second = near_grain[pair_dev, contact_pairs[1]]
    push = contact_force(grain_position[:, first], grain_velocity[:, first], grain_radius[first], grain_position[:, second], grain_velocity[:, second], grain_radius[second])
    contact_total = jax.ops.segment_sum(push.T, first, GRAINS).T
    velocity_next = grain_velocity + (fluid_force + contact_total) / grain_mass[None]
    position_next = grain_position + velocity_next
    return (read, velocity_next, position_next)
```

```python
import jax
import jax.numpy as jnp
from jax import lax
from jax.experimental import pallas as pl
from jax.experimental.pallas import tpu as pltpu
from jax.sharding import PartitionSpec as P

lattice_dirs = (
    (0, 0, 0),
    (1, 0, 0),
    (-1, 0, 0),
    (0, 1, 0),
    (0, -1, 0),
    (0, 0, 1),
    (0, 0, -1),
    (1, 1, 0),
    (-1, -1, 0),
    (1, -1, 0),
    (-1, 1, 0),
    (1, 0, 1),
    (-1, 0, -1),
    (1, 0, -1),
    (-1, 0, 1),
    (0, 1, 1),
    (0, -1, -1),
    (0, 1, -1),
    (0, -1, 1),
)
lattice_weights = (1.0 / 3.0,) + (1.0 / 18.0,) * 6 + (1.0 / 36.0,) * 12
opposite = (0, 2, 1, 4, 3, 6, 5, 8, 7, 10, 9, 12, 11, 14, 13, 16, 15, 18, 17)
relax_rate = 1.25
stiffness = 0.5
damping = 0.5

from_low_x = (1, 7, 9, 11, 13)
from_high_x = (2, 8, 10, 12, 14)
from_low_y = (3, 7, 10, 15, 17)
from_high_y = (4, 8, 9, 16, 18)

fields = ((1, 0, 0), (0, 1, 0), (0, 0, 1), (1, 1, 0), (1, -1, 0), (1, 0, 1), (1, 0, -1), (0, 1, 1), (0, 1, -1))


def field_of(direction):
    vector = lattice_dirs[direction]
    if vector in fields:
        return fields.index(vector), 1.0
    return fields.index(tuple(-c for c in vector)), -1.0


WX, WY, WZ = 8, 8, 128
ROWS = WX * WY
VMEM = pl.BlockSpec(memory_space=pltpu.VMEM)
f32 = jnp.float32
i32 = jnp.int32


def call(kernel, outs, scratch=(), limit=24, flops=1_000_000):
    def run(*args):
        return pl.pallas_call(
            kernel,
            out_shape=[jax.ShapeDtypeStruct(s, d) for s, d in outs],
            in_specs=[VMEM] * len(args),
            out_specs=[VMEM] * len(outs),
            scratch_shapes=list(scratch),
            compiler_params=pltpu.CompilerParams(vmem_limit_bytes=limit << 20),
            cost_estimate=pl.CostEstimate(flops=flops, bytes_accessed=1 << 20, transcendentals=0),
        )(*args)

    return run


def lane_take(table, index):
    return jnp.take_along_axis(table, index, axis=1, mode="promise_in_bounds")


def spread(row):
    return jnp.broadcast_to(row, (8, 128))


def sublane_iota():
    return lax.broadcasted_iota(i32, (8, 128), 0)


def lane_iota():
    return lax.broadcasted_iota(i32, (8, 128), 1)


def collide(pops):
    density = pops[0]
    for direction in range(1, 19):
        density = density + pops[direction]
    inverse = 1.0 / density
    speeds = []
    for compo in range(3):
        moment = None
        for direction in range(1, 19):
            factor = lattice_dirs[direction][compo]
            if factor == 1:
                moment = pops[direction] if moment is None else moment + pops[direction]
            elif factor == -1:
                moment = moment - pops[direction]
        speeds.append(moment * inverse)
    square = speeds[0] * speeds[0] + speeds[1] * speeds[1] + speeds[2] * speeds[2]
    rest = 1.0 - 1.5 * square
    keep = 1.0 - relax_rate
    scaled = relax_rate * density
    post = [None] * 19
    post[0] = keep * pops[0] + (lattice_weights[0] * scaled) * rest
    scale = {w: w * scaled for w in (1.0 / 18.0, 1.0 / 36.0)}
    for direction in range(1, 19, 2):
        along = None
        for compo in range(3):
            factor = lattice_dirs[direction][compo]
            if factor == 1:
                along = speeds[compo] if along is None else along + speeds[compo]
            elif factor == -1:
                along = along - speeds[compo]
        weight = scale[lattice_weights[direction]]
        even = weight * (rest + 4.5 * along * along)
        odd = weight * (3.0 * along)
        post[direction] = keep * pops[direction] + even + odd
        post[direction + 1] = keep * pops[direction + 1] + even - odd
    total = post[0]
    for direction in range(1, 19):
        total = total + post[direction]
    return post, total


def first_kernel(pop, ids, near, g, r, x_up, x_down, y_up, y_down, ask):
    lane = lane_iota()
    sub = sublane_iota()
    for tile in range(16):
        row = near[0:1, (tile // 2) * 128 : (tile // 2) * 128 + 128]
        index = (8 * (tile % 2) + sub) * 8 + (lane & 7)
        ask[tile * 8 : tile * 8 + 8, :] = lane_take(spread(row), index)
    for x in range(WX):
        pops = [pop[c * ROWS + x * 8 : c * ROWS + x * 8 + 8, :] for c in range(19)]
        cell = ids[x * 8 : x * 8 + 8, :]
        fluid = cell < 0
        post, total = collide(pops)
        post = [jnp.where(fluid, p, 0.0) for p in post]
        total = jnp.where(fluid, total, 0.0)
        for c in range(19):
            g[c * ROWS + x * 8 : c * ROWS + x * 8 + 8, :] = post[c]
        r[x * 8 : x * 8 + 8, :] = total
        for at, names, out in ((WX - 1, from_low_x, x_up), (0, from_high_x, x_down)):
            if x == at:
                for k, c in enumerate(names):
                    out[k * 8 : k * 8 + 8, :] = post[c]
                out[40:48, :] = total
                out[48:56, :] = cell.astype(f32)
    for y, names, out in ((WY - 1, from_low_y, y_up), (0, from_high_y, y_down)):
        for k, c in enumerate(names):
            out[k * 8 : k * 8 + 8, :] = g[pl.ds(c * ROWS + y, 8, stride=8), :]
        out[40:48, :] = r[pl.ds(y, 8, stride=8), :]
        out[48:56, :] = ids[pl.ds(y, 8, stride=8), :].astype(f32)


def corner_kernel(y_up, y_down, low, high, out_up, out_down):
    zero = jnp.zeros((2, 128), f32)
    for src, out, y, k_low, k_high in (
        (y_up, out_up, WY - 1, from_low_x.index(7), from_high_x.index(10)),
        (y_down, out_down, 0, from_low_x.index(9), from_high_x.index(8)),
    ):
        out[0:56, :] = src[...]
        for at, halo, k in ((56, low, k_low), (59, high, k_high)):
            out[at : at + 1, :] = halo[k * 8 + y : k * 8 + y + 1, :]
            out[at + 1 : at + 2, :] = halo[40 + y : 41 + y, :]
            out[at + 2 : at + 3, :] = halo[48 + y : 49 + y, :]
        out[62:64, :] = zero


def shift_y(value, c_y, row):
    sub = sublane_iota()
    if c_y == 1:
        return jnp.where(sub == 0, spread(row), pltpu.roll(value, 1, 0))
    return jnp.where(sub == WY - 1, spread(row), pltpu.roll(value, WY - 1, 0))


def shift_z(value, c_z):
    return value if c_z == 0 else pltpu.roll(value, c_z % WZ, 1)


def stencil_kernel(g, r, pop, ids, low, high, y_low, y_high, base, sums, shifted, part, left, hot):
    def y_row(c_y, k, x):
        halo = y_low if c_y == 1 else y_high
        if x == -1:
            at = 56 + (1 if k is None else 0)
        elif x == WX:
            at = 59 + (1 if k is None else 0)
        else:
            at = (5 if k is None else k) * 8 + x
        return halo[at : at + 1, :]

    def source(direction, x):
        c_x, c_y, c_z = lattice_dirs[direction]
        at = x - c_x
        if at == -1:
            k = from_low_x.index(direction)
            value = low[k * 8 : k * 8 + 8, :]
        elif at == WX:
            k = from_high_x.index(direction)
            value = high[k * 8 : k * 8 + 8, :]
        else:
            value = g[direction * ROWS + at * 8 : direction * ROWS + at * 8 + 8, :]
        if c_y != 0:
            k = (from_low_y if c_y == 1 else from_high_y).index(direction)
            value = shift_y(value, c_y, y_row(c_y, k, at))
        return shift_z(value, c_z)

    combos = [(0, 0), (1, 0), (-1, 0), (0, 1), (0, -1), (1, 1), (-1, -1), (1, -1), (-1, 1)]
    for at in range(-1, WX + 1):
        plain = low[40:48, :] if at == -1 else high[40:48, :] if at == WX else r[at * 8 : at * 8 + 8, :]
        by_y = {0: plain}
        for c_y in (1, -1):
            by_y[c_y] = shift_y(plain, c_y, y_row(c_y, None, at))
        for k, (c_y, c_z) in enumerate(combos):
            if c_y != 0 and c_z != 0 and not 0 <= at < WX:
                continue
            shifted[k * 80 + (at + 1) * 8 : k * 80 + (at + 1) * 8 + 8, :] = shift_z(by_y[c_y], c_z)

    sub = sublane_iota()
    total = jnp.zeros((160, 128), f32)
    for x in range(WX):
        rows = slice(x * 8, x * 8 + 8)
        cell = ids[rows, :]
        fluid = cell < 0
        base[x * 8 : x * 8 + 8, :] = jnp.where(fluid, g[x * 8 : x * 8 + 8, :], pop[x * 8 : x * 8 + 8, :])
        acc = [None] * 9

        def add(k, value):
            acc[k] = value if acc[k] is None else acc[k] + value

        for direction in range(1, 19):
            vector = lattice_dirs[direction]
            c_x, c_y, c_z = vector
            k = combos.index((c_y, c_z))
            near_r = shifted[k * 80 + (x - c_x + 1) * 8 : k * 80 + (x - c_x + 1) * 8 + 8, :]
            came = source(direction, x)
            at = direction * ROWS + x * 8
            back = opposite[direction] * ROWS + x * 8
            open_link = jnp.where(near_r != 0.0, came, g[back : back + 8, :])
            base[at : at + 8, :] = jnp.where(fluid, open_link, pop[at : at + 8, :])
            pull = (-6.0 * lattice_weights[direction]) * near_r
            for compo in range(3):
                if vector[compo] == 1:
                    add(compo, came)
                elif vector[compo] == -1:
                    acc[compo] = -came if acc[compo] is None else acc[compo] - came
                if vector[compo] != 0:
                    add(3 + compo, pull)
            for n, (p, q) in enumerate(((0, 1), (0, 2), (1, 2))):
                if vector[p] * vector[q] == 1:
                    add(6 + n, pull)
                elif vector[p] * vector[q] == -1:
                    acc[6 + n] = -pull if acc[6 + n] is None else acc[6 + n] - pull
        for v in range(9):
            value = 2.0 * acc[v] if v < 3 else acc[v]
            head = value.astype(jnp.bfloat16).astype(f32)
            part[v * 8 : v * 8 + 8, :] = head
            part[80 + v * 8 : 80 + v * 8 + 8, :] = value - head
        zero = jnp.zeros((8, 128), f32)
        for y in range(WY):
            key = ids[x * 8 + y : x * 8 + y + 1, :]
            slot = spread(key & 7)
            pick = slot == sub
            for half in range(2):
                rows_v = [
                    jnp.where(pick, spread(part[half * 80 + v * 8 + y : half * 80 + v * 8 + y + 1, :]), 0.0)
                    for v in range(9)
                ] + [zero]
                left[half * 80 : half * 80 + 80, y * 128 : y * 128 + 128] = jnp.concatenate(rows_v, 0).astype(
                    jnp.bfloat16
                )
            owner = jnp.broadcast_to(key >> 3, (128, 128))
            number = lax.broadcasted_iota(i32, (128, 128), 0)
            hot[:, y * 128 : y * 128 + 128] = jnp.where(owner == number, 1.0, 0.0).astype(jnp.bfloat16)
        total = total + lax.dot_general(
            left[...], hot[...], (((1,), (1,)), ((), ())), preferred_element_type=f32
        )
    sums[...] = total[0:72, :] + total[80:152, :]


def reply_kernel(got, pos, vel, rad, sums, out, rows_t):
    rows = got[...].astype(f32).T[0:8, :].astype(i32)
    rows_t[...] = rows
    chunk = rows >> 7
    index = rows & 127
    state = []
    for ref, count in ((pos, 3), (vel, 3), (rad, 1)):
        for c in range(count):
            value = jnp.zeros((8, 128), f32)
            for k in range(4):
                table = spread(ref[c : c + 1, k * 128 : k * 128 + 128])
                value = jnp.where(chunk == k, lane_take(table, index), value)
            state.append(value)
    out[pl.ds(0, 128, stride=2), :] = jnp.concatenate(state + [sums[...]], 0).T
    lane = lane_iota()
    side = {-1: (lane & -8) | ((lane - 1) & 7), 1: (lane & -8) | ((lane + 1) & 7)}

    def moved(value, d_x, d_y):
        if d_x != 0:
            value = pltpu.roll(value, 8 if d_x == -1 else 120, 1)
        return value if d_y == 0 else lane_take(value, side[d_y])

    speed = state[3:6]
    plus = speed[0] + speed[1]
    minus = speed[0] - speed[1]
    rest = []
    for d_x, d_y in ((-1, 0), (1, 0), (0, -1), (0, 1)):
        rest += [moved(value, d_x, d_y) for value in speed]
    for d_x, d_y, value in ((-1, -1, plus), (-1, 1, minus), (1, -1, minus), (1, 1, plus)):
        rest.append(moved(value, d_x, d_y))
    out[pl.ds(1, 128, stride=2), :] = jnp.concatenate(rest, 0).T


def last_kernel(
    got, rows_t, base, r, ids, low, high, y_low, y_high, pairs, pos, vel, rad, mass,
    read, vel_next, pos_next,
    table, around, moving, rim, left, hot, pair,
):
    table[...] = got[pl.ds(0, 128, stride=2), :].T
    around[...] = got[pl.ds(1, 128, stride=2), :].T

    def look_up(ref, starts, cell):
        owner = (cell >> 3) & 127
        slot = jnp.where(cell >= 0, cell & 7, 8)
        values = [jnp.zeros((8, 128), f32) for start in starts]
        for s in range(8):
            chosen = slot == s
            for n, start in enumerate(starts):
                taken = lane_take(spread(ref[start + s : start + s + 1, :]), owner)
                values[n] = jnp.where(chosen, taken, values[n])
        return values

    def combine(values, vector):
        total = None
        for value, factor in zip(values, vector):
            if factor == 1:
                total = value if total is None else total + value
            elif factor == -1:
                total = total - value
        return total

    for x in range(WX):
        speeds = look_up(table, (24, 32, 40), ids[x * 8 : x * 8 + 8, :])
        for n, vector in enumerate(fields):
            moving[n * 80 + (x + 1) * 8 : n * 80 + (x + 1) * 8 + 8, :] = combine(speeds, vector)
    for at, halo, start in ((-1, low, 0), (WX, high, 24)):
        speeds = look_up(around, (start, start + 8, start + 16), halo[48:56, :].astype(i32))
        for n, vector in enumerate(fields):
            if vector[0] != 0:
                moving[n * 80 + (at + 1) * 8 : n * 80 + (at + 1) * 8 + 8, :] = combine(speeds, vector)
    for side, halo, start, first, second in ((0, y_low, 48, 96, 112), (1, y_high, 72, 104, 120)):
        speeds = look_up(around, (start, start + 8, start + 16), halo[48:56, :].astype(i32))
        for n, vector in enumerate(fields):
            if vector[1] != 0:
                rim[side * 88 + n * 8 : side * 88 + n * 8 + 8, :] = combine(speeds, vector)
        for n, (row, start_row) in enumerate(((58, first), (61, second))):
            (value,) = look_up(around, (start_row,), spread(halo[row : row + 1, :]).astype(i32))
            rim[side * 88 + 72 + n * 8 : side * 88 + 80 + n * 8, :] = value

    for x in range(WX):
        mine = r[x * 8 : x * 8 + 8, :]
        read[x * 8 : x * 8 + 8, :] = base[x * 8 : x * 8 + 8, :]
        for direction in range(1, 19):
            c_x, c_y, c_z = lattice_dirs[direction]
            n, sign = field_of(direction)
            at = x - c_x
            value = moving[n * 80 + (at + 1) * 8 : n * 80 + (at + 1) * 8 + 8, :]
            if c_y != 0:
                side = 0 if c_y == 1 else 1
                row = side * 88 + (72 if at == -1 else 80 if at == WX else n * 8 + at)
                value = shift_y(value, c_y, rim[row : row + 1, :])
            value = shift_z(value, c_z)
            to = direction * ROWS + x * 8
            read[to : to + 8, :] = base[to : to + 8, :] + ((sign * 6.0 * lattice_weights[direction]) * mine) * value

    for k in range(8):
        pair[k : k + 1, :] = pairs[0:1, k * 128 : k * 128 + 128]
        pair[8 + k : 9 + k, :] = pairs[1:2, k * 128 : k * 128 + 128]
    first = pair[0:8, :]
    second = pair[8:16, :]
    chunk = first >> 7
    index = first & 127
    state_a = []
    for ref, count in ((pos, 3), (vel, 3), (rad, 1)):
        for c in range(count):
            value = jnp.zeros((8, 128), f32)
            for k in range(4):
                value = jnp.where(
                    chunk == k, lane_take(spread(ref[c : c + 1, k * 128 : k * 128 + 128]), index), value
                )
            state_a.append(value)
    state_b = look_up(table, tuple(8 * c for c in range(7)), second)
    offset = [a - b for a, b in zip(state_a[0:3], state_b[0:3])]
    length = jnp.sqrt(offset[0] * offset[0] + offset[1] * offset[1] + offset[2] * offset[2])
    inverse = 1.0 / jnp.maximum(length, 1.0)
    normal = [o * inverse for o in offset]
    inter = jnp.maximum(state_a[6] + state_b[6] - length, 0.0)
    closing = None
    for a, b, n in zip(state_a[3:6], state_b[3:6], normal):
        closing = (a - b) * n if closing is None else closing + (a - b) * n
    size = stiffness * inter - damping * inter * closing
    push = [size * n for n in normal]

    left[...] = jnp.zeros((16, 2048), f32)
    number = lax.broadcasted_iota(i32, (512, 128), 0)
    for s in range(8):
        left[0:9, s * 128 : s * 128 + 128] = table[pl.ds(56 + s, 9, stride=8), :]
        key = jnp.broadcast_to(rows_t[s : s + 1, :], (512, 128))
        hot[:, s * 128 : s * 128 + 128] = jnp.where(key == number, 1.0, 0.0).astype(jnp.bfloat16)
    for k in range(8):
        columns = slice(1024 + k * 128, 1024 + k * 128 + 128)
        for c in range(3):
            left[9 + c : 10 + c, columns] = push[c][k : k + 1, :]
        key = jnp.broadcast_to(pairs[0:1, k * 128 : k * 128 + 128], (512, 128))
        hot[:, columns] = jnp.where(key == number, 1.0, 0.0).astype(jnp.bfloat16)
    values = left[...]
    head = values.astype(jnp.bfloat16)
    tail = (values - head.astype(f32)).astype(jnp.bfloat16)
    by_grain = lax.dot_general(
        jnp.concatenate([head, tail], 0), hot[...], (((1,), (1,)), ((), ())), preferred_element_type=f32
    )
    by_grain = by_grain[0:16, :] + by_grain[16:32, :]
    part = [by_grain[n : n + 1, :] for n in range(12)]
    speed = [vel[c : c + 1, :] for c in range(3)]
    matrix = ((3, 6, 7), (6, 4, 8), (7, 8, 5))
    for c in range(3):
        force = part[c]
        for q in range(3):
            force = force + part[matrix[c][q]] * speed[q]
        fresh = speed[c] + (force + part[9 + c]) / mass[...]
        vel_next[c : c + 1, :] = fresh
        pos_next[c : c + 1, :] = pos[c : c + 1, :] + fresh


def ring(axis, value, up):
    count = lax.axis_size(axis)
    pairs = [(i, (i + 1) % count) if up else ((i + 1) % count, i) for i in range(count)]
    return lax.ppermute(value, axis, pairs)


def exchange(value):
    return lax.all_to_all(value, ("gx", "yz"), split_axis=0, concat_axis=0, tiled=True)


def local(
    populations,
    cell_grain,
    near_rows,
    contact_pairs,
    grain_position,
    grain_velocity,
    grain_radius,
    grain_mass,
):
    pop = populations.reshape(19 * ROWS, 128)
    ids = cell_grain.reshape(ROWS, 128)
    rad = grain_radius.reshape(1, 512)
    mass = grain_mass.reshape(1, 512)
    slab = (56, 128)
    full = (19 * ROWS, 128)
    g, r, x_up, x_down, y_up, y_down, ask = call(
        first_kernel,
        [(full, f32), ((ROWS, 128), f32), (slab, f32), (slab, f32), (slab, f32), (slab, f32), ((128, 128), i32)],
    )(pop, ids, near_rows)
    low = ring("gx", x_up, True)
    high = ring("gx", x_down, False)
    asked = exchange(ask)
    y_up, y_down = call(corner_kernel, [((64, 128), f32), ((64, 128), f32)])(y_up, y_down, low, high)
    y_low = ring("yz", y_up, True)
    y_high = ring("yz", y_down, False)
    base, sums = call(
        stencil_kernel,
        [(full, f32), ((72, 128), f32)],
        [
            pltpu.VMEM((9 * 80, 128), f32),
            pltpu.VMEM((160, 128), f32),
            pltpu.VMEM((160, 1024), jnp.bfloat16),
            pltpu.VMEM((128, 1024), jnp.bfloat16),
        ],
    )(g, r, pop, ids, low, high, y_low, y_high)
    send, rows_t = call(reply_kernel, [((256, 128), f32), ((8, 128), i32)])(
        asked, grain_position, grain_velocity, rad, sums
    )
    got = exchange(send.reshape(128, 2, 128)).reshape(256, 128)
    read, vel_next, pos_next = call(
        last_kernel,
        [(full, f32), ((3, 512), f32), ((3, 512), f32)],
        [
            pltpu.VMEM((128, 128), f32),
            pltpu.VMEM((128, 128), f32),
            pltpu.VMEM((9 * 80, 128), f32),
            pltpu.VMEM((2 * 88, 128), f32),
            pltpu.VMEM((16, 2048), f32),
            pltpu.VMEM((512, 2048), jnp.bfloat16),
            pltpu.VMEM((16, 128), i32),
        ],
    )(got, rows_t, base, r, ids, low, high, y_low, y_high, contact_pairs, grain_position, grain_velocity, rad, mass)
    return (read.reshape(19, WX, WY, WZ), vel_next, pos_next)


def solution(mesh):
    return jax.shard_map(
        local,
        mesh=mesh,
        in_specs=(
            P(None, "gx", "yz", None),
            P("gx", "yz", None),
            P(("gx", "yz"), None),
            P(None, ("gx", "yz")),
            P(None, ("gx", "yz")),
            P(None, ("gx", "yz")),
            P(("gx", "yz")),
            P(("gx", "yz")),
        ),
        out_specs=(P(None, "gx", "yz", None), P(None, ("gx", "yz")), P(None, ("gx", "yz"))),
        check_vma=False,
    )
```

```python
import jax
import jax.numpy as jnp
from jax import lax
from jax.experimental import pallas as pl
from jax.experimental.pallas import tpu as pltpu
from jax.sharding import PartitionSpec as P


lattice_dirs = (
    (0, 0, 0),
    (1, 0, 0),
    (-1, 0, 0),
    (0, 1, 0),
    (0, -1, 0),
    (0, 0, 1),
    (0, 0, -1),
    (1, 1, 0),
    (-1, -1, 0),
    (1, -1, 0),
    (-1, 1, 0),
    (1, 0, 1),
    (-1, 0, -1),
    (1, 0, -1),
    (-1, 0, 1),
    (0, 1, 1),
    (0, -1, -1),
    (0, 1, -1),
    (0, -1, 1),
)
lattice_weights = (1.0 / 3.0,) + (1.0 / 18.0,) * 6 + (1.0 / 36.0,) * 12
opposite = (0, 2, 1, 4, 3, 6, 5, 8, 7, 10, 9, 12, 11, 14, 13, 16, 15, 18, 17)
relax_rate = 1.25
stiffness = 0.5
damping = 0.5

from_low_x = (1, 7, 9, 11, 13)
from_high_x = (2, 8, 10, 12, 14)
from_low_y = (3, 7, 10, 15, 17)
from_high_y = (4, 8, 9, 16, 18)

fields = ((1, 0, 0), (0, 1, 0), (0, 0, 1), (1, 1, 0), (1, -1, 0), (1, 0, 1), (1, 0, -1), (0, 1, 1), (0, 1, -1))


def field_of(direction):
    vector = lattice_dirs[direction]
    if vector in fields:
        return fields.index(vector), 1.0
    return fields.index(tuple(-c for c in vector)), -1.0


WX, WY, WZ = 8, 8, 128
ROWS = WX * WY
VMEM = pl.BlockSpec(memory_space=pltpu.VMEM)
HBM = pl.BlockSpec(memory_space=pltpu.HBM)
f32 = jnp.float32
i32 = jnp.int32


def call(kernel, outs, scratch=(), limit=24, flops=1_000_000, in_specs=None, out_specs=None, aliases=None):
    def run(*args):
        return pl.pallas_call(
            kernel,
            out_shape=[jax.ShapeDtypeStruct(s, d) for s, d in outs],
            in_specs=in_specs or [VMEM] * len(args),
            out_specs=out_specs or [VMEM] * len(outs),
            scratch_shapes=list(scratch),
            input_output_aliases=aliases or {},
            compiler_params=pltpu.CompilerParams(vmem_limit_bytes=limit << 20),
            cost_estimate=pl.CostEstimate(flops=flops, bytes_accessed=1 << 20, transcendentals=0),
        )(*args)

    return run


def lane_take(table, index):
    return jnp.take_along_axis(table, index, axis=1, mode="promise_in_bounds")


def spread(row):
    return jnp.broadcast_to(row, (8, 128))


def sublane_iota():
    return lax.broadcasted_iota(i32, (8, 128), 0)


def lane_iota():
    return lax.broadcasted_iota(i32, (8, 128), 1)


def collide(pops):
    density = pops[0]
    for direction in range(1, 19):
        density = density + pops[direction]
    inverse = 1.0 / density
    speeds = []
    for compo in range(3):
        moment = None
        for direction in range(1, 19):
            factor = lattice_dirs[direction][compo]
            if factor == 1:
                moment = pops[direction] if moment is None else moment + pops[direction]
            elif factor == -1:
                moment = moment - pops[direction]
        speeds.append(moment * inverse)
    square = speeds[0] * speeds[0] + speeds[1] * speeds[1] + speeds[2] * speeds[2]
    rest = 1.0 - 1.5 * square
    keep = 1.0 - relax_rate
    scaled = relax_rate * density
    post = [None] * 19
    post[0] = keep * pops[0] + (lattice_weights[0] * scaled) * rest
    scale = {w: w * scaled for w in (1.0 / 18.0, 1.0 / 36.0)}
    for direction in range(1, 19, 2):
        along = None
        for compo in range(3):
            factor = lattice_dirs[direction][compo]
            if factor == 1:
                along = speeds[compo] if along is None else along + speeds[compo]
            elif factor == -1:
                along = along - speeds[compo]
        weight = scale[lattice_weights[direction]]
        even = weight * (rest + 4.5 * along * along)
        odd = weight * (3.0 * along)
        post[direction] = keep * pops[direction] + even + odd
        post[direction + 1] = keep * pops[direction + 1] + even - odd
    total = post[0]
    for direction in range(1, 19):
        total = total + post[direction]
    return post, total


def first_kernel(
    pop_in, ids_in, near_in, pairs_in, pos_in, vel_in, rad_in, mass_in,
    pop, ids, pairs, pos, vel, rad, mass, g, r, x_up, x_down, y_up, y_down, ask_out,
    near, ask, sems,
):
    copies = [
        pltpu.make_async_copy(src, dst, sems.at[k])
        for k, (src, dst) in enumerate(
            (
                (near_in, near),
                (ids_in, ids),
                (pop_in, pop),
                (pairs_in, pairs),
                (pos_in, pos),
                (vel_in, vel),
                (rad_in, rad),
                (mass_in, mass),
            )
        )
    ]
    for copy in copies:
        copy.start()
    copies[0].wait()
    lane = lane_iota()
    sub = sublane_iota()
    for tile in range(16):
        row = near[0:1, (tile // 2) * 128 : (tile // 2) * 128 + 128]
        index = (8 * (tile % 2) + sub) * 8 + (lane & 7)
        ask[tile * 8 : tile * 8 + 8, :] = lane_take(spread(row), index)
    sent = pltpu.make_async_copy(ask, ask_out, sems.at[8])
    sent.start()
    copies[1].wait()
    copies[2].wait()
    for x in range(WX):
        pops = [pop[c * ROWS + x * 8 : c * ROWS + x * 8 + 8, :] for c in range(19)]
        cell = ids[x * 8 : x * 8 + 8, :]
        fluid = cell < 0
        post, total = collide(pops)
        post = [jnp.where(fluid, p, 0.0) for p in post]
        total = jnp.where(fluid, total, 0.0)
        for c in range(19):
            g[c * ROWS + x * 8 : c * ROWS + x * 8 + 8, :] = post[c]
        r[x * 8 : x * 8 + 8, :] = total
        for at, names, out in ((WX - 1, from_low_x, x_up), (0, from_high_x, x_down)):
            if x == at:
                for k, c in enumerate(names):
                    out[k * 8 : k * 8 + 8, :] = post[c]
                out[40:48, :] = total
                out[48:56, :] = cell.astype(f32)
    for y, names, out in ((WY - 1, from_low_y, y_up), (0, from_high_y, y_down)):
        for k, c in enumerate(names):
            out[k * 8 : k * 8 + 8, :] = g[pl.ds(c * ROWS + y, 8, stride=8), :]
        out[40:48, :] = r[pl.ds(y, 8, stride=8), :]
        out[48:56, :] = ids[pl.ds(y, 8, stride=8), :].astype(f32)
    for copy in copies[3:]:
        copy.wait()
    sent.wait()


def corner_kernel(y_up, y_down, low, high, out_up, out_down):
    zero = jnp.zeros((2, 128), f32)
    for src, out, y, k_low, k_high in (
        (y_up, out_up, WY - 1, from_low_x.index(7), from_high_x.index(10)),
        (y_down, out_down, 0, from_low_x.index(9), from_high_x.index(8)),
    ):
        out[0:56, :] = src[...]
        for at, halo, k in ((56, low, k_low), (59, high, k_high)):
            out[at : at + 1, :] = halo[k * 8 + y : k * 8 + y + 1, :]
            out[at + 1 : at + 2, :] = halo[40 + y : 41 + y, :]
            out[at + 2 : at + 3, :] = halo[48 + y : 49 + y, :]
        out[62:64, :] = zero


def shift_y(value, c_y, row):
    sub = sublane_iota()
    if c_y == 1:
        return jnp.where(sub == 0, spread(row), pltpu.roll(value, 1, 0))
    return jnp.where(sub == WY - 1, spread(row), pltpu.roll(value, WY - 1, 0))


def shift_z(value, c_z):
    return value if c_z == 0 else pltpu.roll(value, c_z % WZ, 1)


combos = ((0, 0), (1, 0), (-1, 0), (0, 1), (0, -1), (1, 1), (-1, -1), (1, -1), (-1, 1))


class Totals:
    def __init__(self, start=None):
        self.acc = start or [None] * 9

    def add(self, k, value, sign):
        if self.acc[k] is None:
            self.acc[k] = value if sign == 1 else -value
        else:
            self.acc[k] = self.acc[k] + value if sign == 1 else self.acc[k] - value

    def link(self, direction, came, near_r):
        vector = lattice_dirs[direction]
        pull = (-6.0 * lattice_weights[direction]) * near_r
        for compo in range(3):
            if vector[compo] != 0:
                self.add(compo, came, vector[compo])
                self.add(3 + compo, pull, 1)
        for n, (p, q) in enumerate(((0, 1), (0, 2), (1, 2))):
            if vector[p] * vector[q] != 0:
                self.add(6 + n, pull, vector[p] * vector[q])


def stream(base, g, pop, fluid, direction, x, came, near_r):
    at = direction * ROWS + x * 8
    back = opposite[direction] * ROWS + x * 8
    open_link = jnp.where(near_r != 0.0, came, g[back : back + 8, :])
    base[at : at + 8, :] = jnp.where(fluid, open_link, pop[at : at + 8, :])


def source_plane(g, low, high, direction, at):
    if at == -1:
        k = from_low_x.index(direction)
        return low[k * 8 : k * 8 + 8, :]
    if at == WX:
        k = from_high_x.index(direction)
        return high[k * 8 : k * 8 + 8, :]
    return g[direction * ROWS + at * 8 : direction * ROWS + at * 8 + 8, :]


def density_plane(r, low, high, at):
    return low[40:48, :] if at == -1 else high[40:48, :] if at == WX else r[at * 8 : at * 8 + 8, :]


def early_kernel(g, r, pop, ids, low, high, pairs, pos, vel, rad, base, forces, hot, pair_hot, state, shifted, pair):
    for at in range(-1, WX + 1):
        plain = density_plane(r, low, high, at)
        for k, c_z in enumerate((0, 1, -1)):
            shifted[k * 80 + (at + 1) * 8 : k * 80 + (at + 1) * 8 + 8, :] = shift_z(plain, c_z)
    for x in range(WX):
        fluid = ids[x * 8 : x * 8 + 8, :] < 0
        base[x * 8 : x * 8 + 8, :] = jnp.where(fluid, g[x * 8 : x * 8 + 8, :], pop[x * 8 : x * 8 + 8, :])
        sums = Totals()
        for direction in range(1, 19):
            c_x, c_y, c_z = lattice_dirs[direction]
            if c_y != 0:
                continue
            at = x - c_x
            row = (0, 1, -1).index(c_z) * 80 + (at + 1) * 8
            near_r = shifted[row : row + 8, :]
            came = shift_z(source_plane(g, low, high, direction, at), c_z)
            stream(base, g, pop, fluid, direction, x, came, near_r)
            sums.link(direction, came, near_r)
        for v in (0, 2, 3, 5, 7):
            forces[v * ROWS + x * 8 : v * ROWS + x * 8 + 8, :] = sums.acc[v]
    number = lax.broadcasted_iota(i32, (128, 128), 0)
    for row in range(ROWS):
        owner = jnp.broadcast_to(ids[row : row + 1, :] >> 3, (128, 128))
        hot[:, row * 128 : row * 128 + 128] = jnp.where(owner == number, 1.0, 0.0).astype(jnp.bfloat16)
    number = lax.broadcasted_iota(i32, (512, 128), 0)
    for k in range(8):
        pair[k : k + 1, :] = pairs[0:1, k * 128 : k * 128 + 128]
        key = jnp.broadcast_to(pairs[0:1, k * 128 : k * 128 + 128], (512, 128))
        pair_hot[:, k * 128 : k * 128 + 128] = jnp.where(key == number, 1.0, 0.0).astype(jnp.bfloat16)
    first = pair[...]
    held = held_states(pos, vel, rad, first >> 7, first & 127)
    for c, value in enumerate(held):
        state[c * 8 : c * 8 + 8, :] = value


def held_states(pos, vel, rad, chunk, index):
    state = []
    for ref, count in ((pos, 3), (vel, 3), (rad, 1)):
        for c in range(count):
            value = jnp.zeros((8, 128), f32)
            for k in range(4):
                table = spread(ref[c : c + 1, k * 128 : k * 128 + 128])
                value = jnp.where(chunk == k, lane_take(table, index), value)
            state.append(value)
    return state


def stencil_kernel(g, r, pop, ids, low, high, y_low, y_high, forces, hot, base_in, base, sums, shifted, part, left):
    def y_row(c_y, k, x):
        halo = y_low if c_y == 1 else y_high
        if x == -1:
            at = 56 + (1 if k is None else 0)
        elif x == WX:
            at = 59 + (1 if k is None else 0)
        else:
            at = (5 if k is None else k) * 8 + x
        return halo[at : at + 1, :]

    def source(direction, x):
        c_x, c_y, c_z = lattice_dirs[direction]
        at = x - c_x
        value = source_plane(g, low, high, direction, at)
        k = (from_low_y if c_y == 1 else from_high_y).index(direction)
        return shift_z(shift_y(value, c_y, y_row(c_y, k, at)), c_z)

    for at in range(-1, WX + 1):
        plain = density_plane(r, low, high, at)
        for c_y in (1, -1):
            value = shift_y(plain, c_y, y_row(c_y, None, at))
            for c_z in (0, 1, -1):
                if c_z == 0 or 0 <= at < WX:
                    k = combos.index((c_y, c_z))
                    shifted[k * 80 + (at + 1) * 8 : k * 80 + (at + 1) * 8 + 8, :] = shift_z(value, c_z)

    sub = sublane_iota()
    total = jnp.zeros((160, 128), f32)
    for x in range(WX):
        fluid = ids[x * 8 : x * 8 + 8, :] < 0
        acc = [None] * 9
        for v in (0, 2, 3, 5, 7):
            acc[v] = forces[v * ROWS + x * 8 : v * ROWS + x * 8 + 8, :]
        links = Totals(acc)
        for direction in range(1, 19):
            c_x, c_y, c_z = lattice_dirs[direction]
            if c_y == 0:
                continue
            row = combos.index((c_y, c_z)) * 80 + (x - c_x + 1) * 8
            near_r = shifted[row : row + 8, :]
            came = source(direction, x)
            stream(base, g, pop, fluid, direction, x, came, near_r)
            links.link(direction, came, near_r)
        for v in range(9):
            value = 2.0 * links.acc[v] if v < 3 else links.acc[v]
            head = value.astype(jnp.bfloat16).astype(f32)
            part[v * 8 : v * 8 + 8, :] = head
            part[80 + v * 8 : 80 + v * 8 + 8, :] = value - head
        zero = jnp.zeros((8, 128), f32)
        for y in range(WY):
            key = ids[x * 8 + y : x * 8 + y + 1, :]
            pick = spread(key & 7) == sub
            for half in range(2):
                rows_v = [
                    jnp.where(pick, spread(part[half * 80 + v * 8 + y : half * 80 + v * 8 + y + 1, :]), 0.0)
                    for v in range(9)
                ] + [zero]
                left[half * 80 : half * 80 + 80, y * 128 : y * 128 + 128] = jnp.concatenate(rows_v, 0).astype(
                    jnp.bfloat16
                )
        total = total + lax.dot_general(
            left[...],
            hot[:, x * 1024 : x * 1024 + 1024],
            (((1,), (1,)), ((), ())),
            preferred_element_type=f32,
        )
    sums[...] = total[0:72, :] + total[80:152, :]


def reply_kernel(got, pos, vel, rad, sums, out, rows_t):
    rows = got[...].astype(f32).T[0:8, :].astype(i32)
    rows_t[...] = rows
    state = held_states(pos, vel, rad, rows >> 7, rows & 127)
    out[pl.ds(0, 128, stride=2), :] = jnp.concatenate(state + [sums[...]], 0).T
    lane = lane_iota()
    side = {-1: (lane & -8) | ((lane - 1) & 7), 1: (lane & -8) | ((lane + 1) & 7)}

    def moved(value, d_x, d_y):
        if d_x != 0:
            value = pltpu.roll(value, 8 if d_x == -1 else 120, 1)
        return value if d_y == 0 else lane_take(value, side[d_y])

    speed = state[3:6]
    plus = speed[0] + speed[1]
    minus = speed[0] - speed[1]
    rest = []
    for d_x, d_y in ((-1, 0), (1, 0), (0, -1), (0, 1)):
        rest += [moved(value, d_x, d_y) for value in speed]
    for d_x, d_y, value in ((-1, -1, plus), (-1, 1, minus), (1, -1, minus), (1, 1, plus)):
        rest.append(moved(value, d_x, d_y))
    out[pl.ds(1, 128, stride=2), :] = jnp.concatenate(rest, 0).T


def last_kernel(
    got, rows_t, base, r, ids, low, high, y_low, y_high, pairs, pair_hot, state, pos, vel, mass,
    read_out, vel_next, pos_next,
    read, table, around, moving, rim, left, hot, pair, sem,
):
    table[...] = got[pl.ds(0, 128, stride=2), :].T
    around[...] = got[pl.ds(1, 128, stride=2), :].T

    def look_up(ref, starts, cell):
        owner = (cell >> 3) & 127
        slot = jnp.where(cell >= 0, cell & 7, 8)
        values = [jnp.zeros((8, 128), f32) for start in starts]
        for s in range(8):
            chosen = slot == s
            for n, start in enumerate(starts):
                taken = lane_take(spread(ref[start + s : start + s + 1, :]), owner)
                values[n] = jnp.where(chosen, taken, values[n])
        return values

    def combine(values, vector):
        total = None
        for value, factor in zip(values, vector):
            if factor == 1:
                total = value if total is None else total + value
            elif factor == -1:
                total = total - value
        return total

    for x in range(WX):
        speeds = look_up(table, (24, 32, 40), ids[x * 8 : x * 8 + 8, :])
        for n, vector in enumerate(fields):
            moving[n * 80 + (x + 1) * 8 : n * 80 + (x + 1) * 8 + 8, :] = combine(speeds, vector)
    for at, halo, start in ((-1, low, 0), (WX, high, 24)):
        speeds = look_up(around, (start, start + 8, start + 16), halo[48:56, :].astype(i32))
        for n, vector in enumerate(fields):
            if vector[0] != 0:
                moving[n * 80 + (at + 1) * 8 : n * 80 + (at + 1) * 8 + 8, :] = combine(speeds, vector)
    for side, halo, start, first, second in ((0, y_low, 48, 96, 112), (1, y_high, 72, 104, 120)):
        speeds = look_up(around, (start, start + 8, start + 16), halo[48:56, :].astype(i32))
        for n, vector in enumerate(fields):
            if vector[1] != 0:
                rim[side * 88 + n * 8 : side * 88 + n * 8 + 8, :] = combine(speeds, vector)
        for n, (row, start_row) in enumerate(((58, first), (61, second))):
            (value,) = look_up(around, (start_row,), spread(halo[row : row + 1, :]).astype(i32))
            rim[side * 88 + 72 + n * 8 : side * 88 + 80 + n * 8, :] = value

    for x in range(WX):
        mine = r[x * 8 : x * 8 + 8, :]
        read[x * 8 : x * 8 + 8, :] = base[x * 8 : x * 8 + 8, :]
        for direction in range(1, 19):
            c_x, c_y, c_z = lattice_dirs[direction]
            n, sign = field_of(direction)
            at = x - c_x
            value = moving[n * 80 + (at + 1) * 8 : n * 80 + (at + 1) * 8 + 8, :]
            if c_y != 0:
                side = 0 if c_y == 1 else 1
                row = side * 88 + (72 if at == -1 else 80 if at == WX else n * 8 + at)
                value = shift_y(value, c_y, rim[row : row + 1, :])
            value = shift_z(value, c_z)
            to = direction * ROWS + x * 8
            read[to : to + 8, :] = base[to : to + 8, :] + ((sign * 6.0 * lattice_weights[direction]) * mine) * value

    sent = pltpu.make_async_copy(read, read_out, sem)
    sent.start()

    for k in range(8):
        pair[k : k + 1, :] = pairs[1:2, k * 128 : k * 128 + 128]
    second = pair[...]
    state_a = [state[c * 8 : c * 8 + 8, :] for c in range(7)]
    state_b = look_up(table, tuple(8 * c for c in range(7)), second)
    offset = [a - b for a, b in zip(state_a[0:3], state_b[0:3])]
    length = jnp.sqrt(offset[0] * offset[0] + offset[1] * offset[1] + offset[2] * offset[2])
    inverse = 1.0 / jnp.maximum(length, 1.0)
    normal = [o * inverse for o in offset]
    inter = jnp.maximum(state_a[6] + state_b[6] - length, 0.0)
    closing = None
    for a, b, n in zip(state_a[3:6], state_b[3:6], normal):
        closing = (a - b) * n if closing is None else closing + (a - b) * n
    size = stiffness * inter - damping * inter * closing
    push = [size * n for n in normal]

    left[...] = jnp.zeros((16, 2048), f32)
    number = lax.broadcasted_iota(i32, (512, 128), 0)
    for s in range(8):
        left[0:9, s * 128 : s * 128 + 128] = table[pl.ds(56 + s, 9, stride=8), :]
        key = jnp.broadcast_to(rows_t[s : s + 1, :], (512, 128))
        hot[:, s * 128 : s * 128 + 128] = jnp.where(key == number, 1.0, 0.0).astype(jnp.bfloat16)
    for k in range(8):
        columns = slice(1024 + k * 128, 1024 + k * 128 + 128)
        for c in range(3):
            left[9 + c : 10 + c, columns] = push[c][k : k + 1, :]
    values = left[...]
    head = values.astype(jnp.bfloat16)
    tail = (values - head.astype(f32)).astype(jnp.bfloat16)
    both = jnp.concatenate([head, tail], 0)
    by_grain = lax.dot_general(both[:, 0:1024], hot[...], (((1,), (1,)), ((), ())), preferred_element_type=f32)
    by_grain = by_grain + lax.dot_general(
        both[:, 1024:2048], pair_hot[...], (((1,), (1,)), ((), ())), preferred_element_type=f32
    )
    by_grain = by_grain[0:16, :] + by_grain[16:32, :]
    part = [by_grain[n : n + 1, :] for n in range(12)]
    speed = [vel[c : c + 1, :] for c in range(3)]
    matrix = ((3, 6, 7), (6, 4, 8), (7, 8, 5))
    for c in range(3):
        force = part[c]
        for q in range(3):
            force = force + part[matrix[c][q]] * speed[q]
        fresh = speed[c] + (force + part[9 + c]) / mass[...]
        vel_next[c : c + 1, :] = fresh
        pos_next[c : c + 1, :] = pos[c : c + 1, :] + fresh
    sent.wait()


def ring(axis, value, up):
    count = lax.axis_size(axis)
    pairs = [(i, (i + 1) % count) if up else ((i + 1) % count, i) for i in range(count)]
    return lax.ppermute(value, axis, pairs)


def exchange(value):
    return lax.all_to_all(value, ("gx", "yz"), split_axis=0, concat_axis=0, tiled=True)


def local(
    populations,
    cell_grain,
    near_rows,
    contact_pairs,
    grain_position,
    grain_velocity,
    grain_radius,
    grain_mass,
):
    pop = populations.reshape(19 * ROWS, 128)
    ids = cell_grain.reshape(ROWS, 128)
    rad = grain_radius.reshape(1, 512)
    mass = grain_mass.reshape(1, 512)
    return step(pop, ids, near_rows, contact_pairs, grain_position, grain_velocity, rad, mass)


def step(pop, ids, near_rows, contact_pairs, grain_position, grain_velocity, rad, mass):
    slab = ((56, 128), f32)
    full = ((19 * ROWS, 128), f32)
    cells = (ROWS, 128)
    vector = ((3, 512), f32)
    scalar = ((1, 512), f32)
    bf16 = jnp.bfloat16
    pop, ids, pairs, pos, vel, rad, mass, g, r, x_up, x_down, y_up, y_down, ask = call(
        first_kernel,
        [full, (cells, i32), ((2, 1024), i32), vector, vector, scalar, scalar]
        + [full, (cells, f32), slab, slab, slab, slab, ((128, 128), i32)],
        [pltpu.VMEM((1, 1024), i32), pltpu.VMEM((128, 128), i32), pltpu.SemaphoreType.DMA((9,))],
        in_specs=[HBM] * 8,
        out_specs=[VMEM] * 13 + [HBM],
    )(*[pltpu.with_memory_space_constraint(v, pltpu.HBM) for v in (pop, ids, near_rows, contact_pairs, grain_position, grain_velocity, rad, mass)])
    low = ring("gx", x_up, True)
    high = ring("gx", x_down, False)
    asked = exchange(ask)
    y_up, y_down = call(corner_kernel, [((64, 128), f32), ((64, 128), f32)])(y_up, y_down, low, high)
    y_low = ring("yz", y_up, True)
    y_high = ring("yz", y_down, False)
    base, forces, hot, pair_hot, state = call(
        early_kernel,
        [full, ((9 * ROWS, 128), f32), ((128, 8192), bf16), ((512, 1024), bf16), ((56, 128), f32)],
        [pltpu.VMEM((240, 128), f32), pltpu.VMEM((8, 128), i32)],
    )(g, r, pop, ids, low, high, pairs, pos, vel, rad)
    base, sums = call(
        stencil_kernel,
        [full, ((72, 128), f32)],
        [pltpu.VMEM((9 * 80, 128), f32), pltpu.VMEM((160, 128), f32), pltpu.VMEM((160, 1024), bf16)],
        aliases={10: 0},
    )(g, r, pop, ids, low, high, y_low, y_high, forces, hot, base)
    send, rows_t = call(reply_kernel, [((256, 128), f32), ((8, 128), i32)])(asked, pos, vel, rad, sums)
    got = exchange(send.reshape(128, 2, 128)).reshape(256, 128)
    read, vel_next, pos_next = call(
        last_kernel,
        [full, vector, vector],
        [
            pltpu.VMEM((19 * ROWS, 128), f32),
            pltpu.VMEM((128, 128), f32),
            pltpu.VMEM((128, 128), f32),
            pltpu.VMEM((9 * 80, 128), f32),
            pltpu.VMEM((2 * 88, 128), f32),
            pltpu.VMEM((16, 2048), f32),
            pltpu.VMEM((512, 1024), bf16),
            pltpu.VMEM((8, 128), i32),
            pltpu.SemaphoreType.DMA,
        ],
        out_specs=[HBM, VMEM, VMEM],
    )(got, rows_t, base, r, ids, low, high, y_low, y_high, pairs, pair_hot, state, pos, vel, mass)
    return (read.reshape(19, WX, WY, WZ), vel_next, pos_next)


def solution(mesh):
    return jax.shard_map(
        local,
        mesh=mesh,
        in_specs=(
            P(None, "gx", "yz", None),
            P("gx", "yz", None),
            P(("gx", "yz"), None),
            P(None, ("gx", "yz")),
            P(None, ("gx", "yz")),
            P(None, ("gx", "yz")),
            P(("gx", "yz")),
            P(("gx", "yz")),
        ),
        out_specs=(P(None, "gx", "yz", None), P(None, ("gx", "yz")), P(None, ("gx", "yz"))),
        check_vma=False,
    )
```

```python
import jax
import jax.numpy as jnp
from jax import lax
from jax.experimental import pallas as pl
from jax.experimental.pallas import tpu as pltpu
from jax.sharding import PartitionSpec as P


lattice_dirs = (
    (0, 0, 0),
    (1, 0, 0),
    (-1, 0, 0),
    (0, 1, 0),
    (0, -1, 0),
    (0, 0, 1),
    (0, 0, -1),
    (1, 1, 0),
    (-1, -1, 0),
    (1, -1, 0),
    (-1, 1, 0),
    (1, 0, 1),
    (-1, 0, -1),
    (1, 0, -1),
    (-1, 0, 1),
    (0, 1, 1),
    (0, -1, -1),
    (0, 1, -1),
    (0, -1, 1),
)
lattice_weights = (1.0 / 3.0,) + (1.0 / 18.0,) * 6 + (1.0 / 36.0,) * 12
opposite = (0, 2, 1, 4, 3, 6, 5, 8, 7, 10, 9, 12, 11, 14, 13, 16, 15, 18, 17)
relax_rate = 1.25
stiffness = 0.5
damping = 0.5

from_low_x = (1, 7, 9, 11, 13)
from_high_x = (2, 8, 10, 12, 14)
from_low_y = (3, 7, 10, 15, 17)
from_high_y = (4, 8, 9, 16, 18)

fields = ((1, 0, 0), (0, 1, 0), (0, 0, 1), (1, 1, 0), (1, -1, 0), (1, 0, 1), (1, 0, -1), (0, 1, 1), (0, 1, -1))


def field_of(direction):
    vector = lattice_dirs[direction]
    if vector in fields:
        return fields.index(vector), 1.0
    return fields.index(tuple(-c for c in vector)), -1.0


WX, WY, WZ = 8, 8, 128
ROWS = WX * WY
VMEM = pl.BlockSpec(memory_space=pltpu.VMEM)
HBM = pl.BlockSpec(memory_space=pltpu.HBM)
f32 = jnp.float32
i32 = jnp.int32


def call(kernel, outs, scratch=(), limit=24, flops=1_000_000, in_specs=None, out_specs=None, aliases=None):
    def run(*args):
        return pl.pallas_call(
            kernel,
            out_shape=[jax.ShapeDtypeStruct(s, d) for s, d in outs],
            in_specs=in_specs or [VMEM] * len(args),
            out_specs=out_specs or [VMEM] * len(outs),
            scratch_shapes=list(scratch),
            input_output_aliases=aliases or {},
            compiler_params=pltpu.CompilerParams(vmem_limit_bytes=limit << 20),
            cost_estimate=pl.CostEstimate(flops=flops, bytes_accessed=1 << 20, transcendentals=0),
        )(*args)

    return run


def lane_take(table, index):
    return jnp.take_along_axis(table, index, axis=1, mode="promise_in_bounds")


def spread(row):
    return jnp.broadcast_to(row, (8, 128))


def sublane_iota():
    return lax.broadcasted_iota(i32, (8, 128), 0)


def lane_iota():
    return lax.broadcasted_iota(i32, (8, 128), 1)


def collide(pops):
    density = pops[0]
    for direction in range(1, 19):
        density = density + pops[direction]
    inverse = 1.0 / density
    speeds = []
    for compo in range(3):
        moment = None
        for direction in range(1, 19):
            factor = lattice_dirs[direction][compo]
            if factor == 1:
                moment = pops[direction] if moment is None else moment + pops[direction]
            elif factor == -1:
                moment = moment - pops[direction]
        speeds.append(moment * inverse)
    square = speeds[0] * speeds[0] + speeds[1] * speeds[1] + speeds[2] * speeds[2]
    rest = 1.0 - 1.5 * square
    keep = 1.0 - relax_rate
    scaled = relax_rate * density
    post = [None] * 19
    post[0] = keep * pops[0] + (lattice_weights[0] * scaled) * rest
    scale = {w: w * scaled for w in (1.0 / 18.0, 1.0 / 36.0)}
    for direction in range(1, 19, 2):
        along = None
        for compo in range(3):
            factor = lattice_dirs[direction][compo]
            if factor == 1:
                along = speeds[compo] if along is None else along + speeds[compo]
            elif factor == -1:
                along = along - speeds[compo]
        weight = scale[lattice_weights[direction]]
        even = weight * (rest + 4.5 * along * along)
        odd = weight * (3.0 * along)
        post[direction] = keep * pops[direction] + even + odd
        post[direction + 1] = keep * pops[direction + 1] + even - odd
    total = post[0]
    for direction in range(1, 19):
        total = total + post[direction]
    return post, total


def first_kernel(
    pop_in, ids_in, near_in, pairs_in, pos_in, vel_in, rad_in, mass_in,
    pop, ids, pairs, pos, vel, rad, mass, g, r, x_up, x_down, y_up, y_down, ask_out,
    near, ask, sems,
):
    def copy(k, src, dst):
        started = pltpu.make_async_copy(src, dst, sems.at[k])
        started.start()
        return started

    asking = copy(0, near_in, near)
    cells = copy(1, ids_in, ids)
    planes = ((0, WX - 1), (1, 2), (3, 4), (5, 6))
    arriving = [
        [copy(2 + 2 * n + m, pop_in.at[:, x], pop.at[:, x]) for m, x in enumerate(chunk)]
        for n, chunk in enumerate(planes)
    ]
    others = [
        copy(10 + k, src, dst)
        for k, (src, dst) in enumerate(
            ((pairs_in, pairs), (pos_in, pos), (vel_in, vel), (rad_in, rad), (mass_in, mass))
        )
    ]
    asking.wait()
    lane = lane_iota()
    sub = sublane_iota()
    for tile in range(16):
        row = near[0:1, (tile // 2) * 128 : (tile // 2) * 128 + 128]
        index = (8 * (tile % 2) + sub) * 8 + (lane & 7)
        ask[tile * 8 : tile * 8 + 8, :] = lane_take(spread(row), index)
    sent = copy(15, ask, ask_out)
    cells.wait()
    for n, x in ((n, x) for n, chunk in enumerate(planes) for x in chunk):
        if x == planes[n][0]:
            for arrival in arriving[n]:
                arrival.wait()
        pops = [pop[c, x] for c in range(19)]
        cell = ids[x * 8 : x * 8 + 8, :]
        fluid = cell < 0
        post, total = collide(pops)
        post = [jnp.where(fluid, p, 0.0) for p in post]
        total = jnp.where(fluid, total, 0.0)
        for c in range(19):
            g[c * ROWS + x * 8 : c * ROWS + x * 8 + 8, :] = post[c]
        r[x * 8 : x * 8 + 8, :] = total
        for at, names, out in ((WX - 1, from_low_x, x_up), (0, from_high_x, x_down)):
            if x == at:
                for k, c in enumerate(names):
                    out[k * 8 : k * 8 + 8, :] = post[c]
                out[40:48, :] = total
                out[48:56, :] = cell.astype(f32)
    for y, names, out in ((WY - 1, from_low_y, y_up), (0, from_high_y, y_down)):
        for k, c in enumerate(names):
            out[k * 8 : k * 8 + 8, :] = g[pl.ds(c * ROWS + y, 8, stride=8), :]
        out[40:48, :] = r[pl.ds(y, 8, stride=8), :]
        out[48:56, :] = ids[pl.ds(y, 8, stride=8), :].astype(f32)
    for other in others:
        other.wait()
    sent.wait()


def corner_kernel(y_up, y_down, low, high, out_up, out_down):
    zero = jnp.zeros((2, 128), f32)
    for src, out, y, k_low, k_high in (
        (y_up, out_up, WY - 1, from_low_x.index(7), from_high_x.index(10)),
        (y_down, out_down, 0, from_low_x.index(9), from_high_x.index(8)),
    ):
        out[0:56, :] = src[...]
        for at, halo, k in ((56, low, k_low), (59, high, k_high)):
            out[at : at + 1, :] = halo[k * 8 + y : k * 8 + y + 1, :]
            out[at + 1 : at + 2, :] = halo[40 + y : 41 + y, :]
            out[at + 2 : at + 3, :] = halo[48 + y : 49 + y, :]
        out[62:64, :] = zero


def shift_y(value, c_y, row):
    sub = sublane_iota()
    if c_y == 1:
        return jnp.where(sub == 0, spread(row), pltpu.roll(value, 1, 0))
    return jnp.where(sub == WY - 1, spread(row), pltpu.roll(value, WY - 1, 0))


def shift_z(value, c_z):
    return value if c_z == 0 else pltpu.roll(value, c_z % WZ, 1)


combos = ((0, 0), (1, 0), (-1, 0), (0, 1), (0, -1), (1, 1), (-1, -1), (1, -1), (-1, 1))


class Totals:
    def __init__(self, start=None):
        self.acc = start or [None] * 9

    def add(self, k, value, sign):
        if self.acc[k] is None:
            self.acc[k] = value if sign == 1 else -value
        else:
            self.acc[k] = self.acc[k] + value if sign == 1 else self.acc[k] - value

    def link(self, direction, came, near_r):
        vector = lattice_dirs[direction]
        pull = (-6.0 * lattice_weights[direction]) * near_r
        for compo in range(3):
            if vector[compo] != 0:
                self.add(compo, came, vector[compo])
                self.add(3 + compo, pull, 1)
        for n, (p, q) in enumerate(((0, 1), (0, 2), (1, 2))):
            if vector[p] * vector[q] != 0:
                self.add(6 + n, pull, vector[p] * vector[q])


def source_plane(g, low, high, direction, at):
    if at == -1:
        k = from_low_x.index(direction)
        return low[k * 8 : k * 8 + 8, :]
    if at == WX:
        k = from_high_x.index(direction)
        return high[k * 8 : k * 8 + 8, :]
    return g[direction * ROWS + at * 8 : direction * ROWS + at * 8 + 8, :]


def density_plane(r, low, high, at):
    return low[40:48, :] if at == -1 else high[40:48, :] if at == WX else r[at * 8 : at * 8 + 8, :]


def spread_slots(part, row, pick):
    halves = []
    for half in range(2):
        rows_v = [
            jnp.where(pick, spread(part[half * 72 + v * 8 + row : half * 72 + v * 8 + row + 1, :]), 0.0) for v in range(9)
        ]
        halves.append(jnp.concatenate(rows_v + [jnp.zeros((8, 128), f32)], 0).astype(jnp.bfloat16))
    return jnp.concatenate(halves, 0)


def split_fields(part, acc):
    for v in range(9):
        if acc[v] is None:
            part[v * 8 : v * 8 + 8, :] = jnp.zeros((8, 128), f32)
            part[72 + v * 8 : 80 + v * 8, :] = jnp.zeros((8, 128), f32)
            continue
        value = 2.0 * acc[v] if v < 3 else acc[v]
        head = value.astype(jnp.bfloat16).astype(f32)
        part[v * 8 : v * 8 + 8, :] = head
        part[72 + v * 8 : 80 + v * 8, :] = value - head


def contract(left, right):
    return lax.dot_general(left, right, (((1,), (1,)), ((), ())), preferred_element_type=f32)


def early_kernel(
    g, r, pop, ids, low, high, pairs, pos, vel, rad,
    base, sums, edge_hot, pair_hot, state,
    shifted, part, left, hot, pair,
):
    sub = sublane_iota()

    def shift(value, c_y, c_z):
        if c_y == 1:
            value = jnp.where(sub == 0, 0.0, pltpu.roll(value, 1, 0))
        elif c_y == -1:
            value = jnp.where(sub == WY - 1, 0.0, pltpu.roll(value, WY - 1, 0))
        return shift_z(value, c_z)

    for at in range(-1, WX + 1):
        plain = density_plane(r, low, high, at)
        for k, (c_y, c_z) in enumerate(combos):
            if 0 <= at < WX or c_y == 0 or c_z == 0:
                shifted[k * 80 + (at + 1) * 8 : k * 80 + (at + 1) * 8 + 8, :] = shift(plain, c_y, c_z)
    number = lax.broadcasted_iota(i32, (128, 128), 0)
    total = jnp.zeros((160, 128), f32)
    for x in range(WX):
        fluid = ids[x * 8 : x * 8 + 8, :] < 0
        base[x * 8 : x * 8 + 8, :] = jnp.where(fluid, g[x * 8 : x * 8 + 8, :], pop[x * 8 : x * 8 + 8, :])
        links = Totals()
        for direction in range(1, 19):
            c_x, c_y, c_z = lattice_dirs[direction]
            row = combos.index((c_y, c_z)) * 80 + (x - c_x + 1) * 8
            near_r = shifted[row : row + 8, :]
            came = shift(source_plane(g, low, high, direction, x - c_x), c_y, c_z)
            at = direction * ROWS + x * 8
            back = opposite[direction] * ROWS + x * 8
            open_link = jnp.where(near_r != 0.0, came, g[back : back + 8, :])
            base[at : at + 8, :] = jnp.where(fluid, open_link, pop[at : at + 8, :])
            links.link(direction, came, near_r)
        split_fields(part, links.acc)
        for y in range(WY):
            key = ids[x * 8 + y : x * 8 + y + 1, :]
            left[:, y * 128 : y * 128 + 128] = spread_slots(part, y, spread(key & 7) == sub)
            owner = jnp.broadcast_to(key >> 3, (128, 128))
            one_hot = jnp.where(owner == number, 1.0, 0.0).astype(jnp.bfloat16)
            hot[:, y * 128 : y * 128 + 128] = one_hot
            if y in (0, WY - 1):
                to = (0 if y == 0 else 1024) + x * 128
                edge_hot[:, to : to + 128] = one_hot
        total = total + contract(left[...], hot[...])
    sums[...] = total[0:72, :] + total[80:152, :]
    for k in range(8):
        key = pairs[0:1, k * 128 : k * 128 + 128]
        pair[k : k + 1, :] = key
        rest = jnp.broadcast_to(key & 127, (128, 128))
        pair_hot[:, k * 128 : k * 128 + 128] = jnp.where(rest == number, 1.0, 0.0).astype(jnp.bfloat16)
    first = pair[...]
    held = held_states(pos, vel, rad, first >> 7, first & 127)
    for c, value in enumerate(held):
        state[c * 8 : c * 8 + 8, :] = value


def complete_rows(ids, y_low, y_high, edge_hot, base, part, left):
    sub = sublane_iota()
    total = jnp.zeros((160, 128), f32)
    for side, (y, halo, names) in enumerate(((0, y_low, from_low_y), (WY - 1, y_high, from_high_y))):
        fluid = ids[pl.ds(y, 8, stride=8), :] < 0
        links = Totals()
        for k, direction in enumerate(names):
            c_x, _, c_z = lattice_dirs[direction]
            came = halo[k * 8 : k * 8 + 8, :]
            near_r = halo[40:48, :]
            if c_x == 1:
                came = jnp.where(sub == 0, spread(halo[56:57, :]), pltpu.roll(came, 1, 0))
                near_r = jnp.where(sub == 0, spread(halo[57:58, :]), pltpu.roll(near_r, 1, 0))
            elif c_x == -1:
                came = jnp.where(sub == WX - 1, spread(halo[59:60, :]), pltpu.roll(came, WX - 1, 0))
                near_r = jnp.where(sub == WX - 1, spread(halo[60:61, :]), pltpu.roll(near_r, WX - 1, 0))
            came = shift_z(came, c_z)
            near_r = shift_z(near_r, c_z)
            at = pl.ds(direction * ROWS + y, 8, stride=8)
            base[at, :] = jnp.where(fluid & (near_r != 0.0), came, base[at, :])
            links.link(direction, came, near_r)
        split_fields(part, links.acc)
        for x in range(WX):
            key = ids[x * 8 + y : x * 8 + y + 1, :]
            left[:, x * 128 : x * 128 + 128] = spread_slots(part, x, spread(key & 7) == sub)
        total = total + contract(left[...], edge_hot[:, side * 1024 : side * 1024 + 1024])
    return total[0:72, :] + total[80:152, :]


def held_states(pos, vel, rad, chunk, index):
    state = []
    for ref, count in ((pos, 3), (vel, 3), (rad, 1)):
        for c in range(count):
            value = jnp.zeros((8, 128), f32)
            for k in range(4):
                table = spread(ref[c : c + 1, k * 128 : k * 128 + 128])
                value = jnp.where(chunk == k, lane_take(table, index), value)
            state.append(value)
    return state


def reply_kernel(
    got, pos, vel, rad, sums, ids, y_low, y_high, edge_hot, base_in, out, rows_t, base, part, left
):
    sums = sums[...] + complete_rows(ids, y_low, y_high, edge_hot, base, part, left)
    rows = got[...].astype(f32).T[0:8, :].astype(i32)
    rows_t[...] = rows
    state = held_states(pos, vel, rad, rows >> 7, rows & 127)
    out[pl.ds(0, 128, stride=2), :] = jnp.concatenate(state + [sums], 0).T
    lane = lane_iota()
    side = {-1: (lane & -8) | ((lane - 1) & 7), 1: (lane & -8) | ((lane + 1) & 7)}

    def moved(value, d_x, d_y):
        if d_x != 0:
            value = pltpu.roll(value, 8 if d_x == -1 else 120, 1)
        return value if d_y == 0 else lane_take(value, side[d_y])

    speed = state[3:6]
    plus = speed[0] + speed[1]
    minus = speed[0] - speed[1]
    rest = []
    for d_x, d_y in ((-1, 0), (1, 0), (0, -1), (0, 1)):
        rest += [moved(value, d_x, d_y) for value in speed]
    for d_x, d_y, value in ((-1, -1, plus), (-1, 1, minus), (1, -1, minus), (1, 1, plus)):
        rest.append(moved(value, d_x, d_y))
    out[pl.ds(1, 128, stride=2), :] = jnp.concatenate(rest, 0).T


def look_up(ref, starts, cell):
    owner = (cell >> 3) & 127
    slot = jnp.where(cell >= 0, cell & 7, 8)
    values = [jnp.zeros((8, 128), f32) for start in starts]
    for s in range(8):
        chosen = slot == s
        for n, start in enumerate(starts):
            taken = lane_take(spread(ref[start + s : start + s + 1, :]), owner)
            values[n] = jnp.where(chosen, taken, values[n])
    return values


def last_kernel(
    got, rows_t, base, r, ids, low, high, y_low, y_high, pairs, pair_hot, state, pos, vel, mass,
    read_out, vel_out, pos_out,
    read, vel_next, pos_next, table, around, moving, rim, left, hot, pair, sems,
):
    table[...] = got[pl.ds(0, 128, stride=2), :].T
    around[...] = got[pl.ds(1, 128, stride=2), :].T

    def combine(values, vector):
        total = None
        for value, factor in zip(values, vector):
            if factor == 1:
                total = value if total is None else total + value
            elif factor == -1:
                total = total - value
        return total

    for x in range(WX):
        speeds = look_up(table, (24, 32, 40), ids[x * 8 : x * 8 + 8, :])
        for n, vector in enumerate(fields):
            moving[n * 80 + (x + 1) * 8 : n * 80 + (x + 1) * 8 + 8, :] = combine(speeds, vector)
    for at, halo, start in ((-1, low, 0), (WX, high, 24)):
        speeds = look_up(around, (start, start + 8, start + 16), halo[48:56, :].astype(i32))
        for n, vector in enumerate(fields):
            if vector[0] != 0:
                moving[n * 80 + (at + 1) * 8 : n * 80 + (at + 1) * 8 + 8, :] = combine(speeds, vector)
    for side, halo, start, first, second in ((0, y_low, 48, 96, 112), (1, y_high, 72, 104, 120)):
        speeds = look_up(around, (start, start + 8, start + 16), halo[48:56, :].astype(i32))
        for n, vector in enumerate(fields):
            if vector[1] != 0:
                rim[side * 88 + n * 8 : side * 88 + n * 8 + 8, :] = combine(speeds, vector)
        for n, (row, start_row) in enumerate(((58, first), (61, second))):
            (value,) = look_up(around, (start_row,), spread(halo[row : row + 1, :]).astype(i32))
            rim[side * 88 + 72 + n * 8 : side * 88 + 80 + n * 8, :] = value

    for x in range(WX):
        mine = r[x * 8 : x * 8 + 8, :]
        read[x * 8 : x * 8 + 8, :] = base[x * 8 : x * 8 + 8, :]
        for direction in range(1, 19):
            c_x, c_y, c_z = lattice_dirs[direction]
            n, sign = field_of(direction)
            at = x - c_x
            value = moving[n * 80 + (at + 1) * 8 : n * 80 + (at + 1) * 8 + 8, :]
            if c_y != 0:
                side = 0 if c_y == 1 else 1
                row = side * 88 + (72 if at == -1 else 80 if at == WX else n * 8 + at)
                value = shift_y(value, c_y, rim[row : row + 1, :])
            value = shift_z(value, c_z)
            to = direction * ROWS + x * 8
            read[to : to + 8, :] = base[to : to + 8, :] + ((sign * 6.0 * lattice_weights[direction]) * mine) * value

    sent = pltpu.make_async_copy(read, read_out, sems.at[0])
    sent.start()

    @pl.when(lax.axis_index("gx") >= 0)
    def _():
        grains(rows_t, pairs, pair_hot, state, pos, vel, mass, vel_next, pos_next, table, left, hot, pair)

    outs = [pltpu.make_async_copy(vel_next, vel_out, sems.at[1]), pltpu.make_async_copy(pos_next, pos_out, sems.at[2])]
    for out in outs:
        out.start()
    for out in outs:
        out.wait()
    sent.wait()


def grains(rows_t, pairs, pair_hot, state, pos, vel, mass, vel_next, pos_next, table, left, hot, pair):
    for k in range(8):
        pair[k : k + 1, :] = pairs[1:2, k * 128 : k * 128 + 128]
    second = pair[...]
    state_a = [state[c * 8 : c * 8 + 8, :] for c in range(7)]
    state_b = look_up(table, tuple(8 * c for c in range(7)), second)
    offset = [a - b for a, b in zip(state_a[0:3], state_b[0:3])]
    length = jnp.sqrt(offset[0] * offset[0] + offset[1] * offset[1] + offset[2] * offset[2])
    inverse = 1.0 / jnp.maximum(length, 1.0)
    normal = [o * inverse for o in offset]
    inter = jnp.maximum(state_a[6] + state_b[6] - length, 0.0)
    closing = None
    for a, b, n in zip(state_a[3:6], state_b[3:6], normal):
        closing = (a - b) * n if closing is None else closing + (a - b) * n
    size = stiffness * inter - damping * inter * closing
    push = [size * n for n in normal]

    sub = sublane_iota()
    number = lax.broadcasted_iota(i32, (128, 128), 0)

    def by_block(values, key):
        pick = spread(key >> 7) == (sub & 3)
        tiles = ([], [])
        for n in range(0, len(values), 2):
            value = spread(values[n])
            if n + 1 < len(values):
                value = jnp.where(sub < 4, value, spread(values[n + 1]))
            value = jnp.where(pick, value, 0.0)
            head = value.astype(jnp.bfloat16).astype(f32)
            tiles[0].append(head)
            tiles[1].append(value - head)
        return jnp.concatenate(tiles[0] + tiles[1], 0).astype(jnp.bfloat16)

    for s in range(8):
        columns = slice(s * 128, s * 128 + 128)
        key = rows_t[s : s + 1, :]
        left[0:80, columns] = by_block([table[56 + v * 8 + s : 57 + v * 8 + s, :] for v in range(9)], key)
        rest = jnp.broadcast_to(jnp.where(key >= 0, key & 127, -1), (128, 128))
        hot[:, columns] = jnp.where(rest == number, 1.0, 0.0).astype(jnp.bfloat16)
        left[80:112, columns] = by_block([p[s : s + 1, :] for p in push], pairs[0:1, columns])
    fluid = contract(left[0:80, :], hot[...])
    fluid = fluid[0:40, :] + fluid[40:80, :]
    contact = contract(left[80:112, :], pair_hot[...])
    contact = contact[0:16, :] + contact[16:32, :]
    matrix = ((3, 6, 7), (6, 4, 8), (7, 8, 5))
    for k in range(4):
        columns = slice(k * 128, k * 128 + 128)
        speed = [vel[c : c + 1, columns] for c in range(3)]
        for c in range(3):
            force = fluid[c * 4 + k : c * 4 + k + 1, :]
            for q in range(3):
                row = matrix[c][q] * 4 + k
                force = force + fluid[row : row + 1, :] * speed[q]
            fresh = speed[c] + (force + contact[c * 4 + k : c * 4 + k + 1, :]) / mass[:, columns]
            vel_next[c : c + 1, columns] = fresh
            pos_next[c : c + 1, columns] = pos[c : c + 1, columns] + fresh


def ring(axis, value, up):
    count = lax.axis_size(axis)
    pairs = [(i, (i + 1) % count) if up else ((i + 1) % count, i) for i in range(count)]
    return lax.ppermute(value, axis, pairs)


def exchange(value):
    return lax.all_to_all(value, ("gx", "yz"), split_axis=0, concat_axis=0, tiled=True)


def local(
    populations,
    cell_grain,
    near_rows,
    contact_pairs,
    grain_position,
    grain_velocity,
    grain_radius,
    grain_mass,
):
    pop = populations
    ids = cell_grain.reshape(ROWS, 128)
    rad = grain_radius.reshape(1, 512)
    mass = grain_mass.reshape(1, 512)
    return step(pop, ids, near_rows, contact_pairs, grain_position, grain_velocity, rad, mass)


def step(pop, ids, near_rows, contact_pairs, grain_position, grain_velocity, rad, mass):
    slab = ((56, 128), f32)
    full = ((19 * ROWS, 128), f32)
    cells = (ROWS, 128)
    vector = ((3, 512), f32)
    scalar = ((1, 512), f32)
    bf16 = jnp.bfloat16
    pop, ids, pairs, pos, vel, rad, mass, g, r, x_up, x_down, y_up, y_down, ask = call(
        first_kernel,
        [((19, WX, WY, WZ), f32), (cells, i32), ((2, 1024), i32), vector, vector, scalar, scalar]
        + [full, (cells, f32), slab, slab, slab, slab, ((128, 128), i32)],
        [pltpu.VMEM((1, 1024), i32), pltpu.VMEM((128, 128), i32), pltpu.SemaphoreType.DMA((16,))],
        in_specs=[HBM] * 8,
        out_specs=[VMEM] * 13 + [HBM],
    )(
        *[
            pltpu.with_memory_space_constraint(value, pltpu.HBM)
            for value in (pop, ids, near_rows, contact_pairs, grain_position, grain_velocity, rad, mass)
        ]
    )
    pop = pop.reshape(19 * ROWS, 128)
    low = ring("gx", x_up, True)
    high = ring("gx", x_down, False)
    asked = exchange(ask)
    y_up, y_down = call(corner_kernel, [((64, 128), f32), ((64, 128), f32)])(y_up, y_down, low, high)
    y_low = ring("yz", y_up, True)
    y_high = ring("yz", y_down, False)
    base, sums, edge_hot, pair_hot, state = call(
        early_kernel,
        [full, ((72, 128), f32), ((128, 2048), bf16), ((128, 1024), bf16), ((56, 128), f32)],
        [
            pltpu.VMEM((9 * 80, 128), f32),
            pltpu.VMEM((144, 128), f32),
            pltpu.VMEM((160, 1024), bf16),
            pltpu.VMEM((128, 1024), bf16),
            pltpu.VMEM((8, 128), i32),
        ],
    )(g, r, pop, ids, low, high, pairs, pos, vel, rad)
    send, rows_t, base = call(
        reply_kernel,
        [((256, 128), f32), ((8, 128), i32), full],
        [pltpu.VMEM((144, 128), f32), pltpu.VMEM((160, 1024), bf16)],
        aliases={9: 2},
    )(asked, pos, vel, rad, sums, ids, y_low, y_high, edge_hot, base)
    got = exchange(send.reshape(128, 2, 128)).reshape(256, 128)
    read, vel_next, pos_next = call(
        last_kernel,
        [full, vector, vector],
        [
            pltpu.VMEM((19 * ROWS, 128), f32),
            pltpu.VMEM((3, 512), f32),
            pltpu.VMEM((3, 512), f32),
            pltpu.VMEM((128, 128), f32),
            pltpu.VMEM((128, 128), f32),
            pltpu.VMEM((9 * 80, 128), f32),
            pltpu.VMEM((2 * 88, 128), f32),
            pltpu.VMEM((112, 1024), bf16),
            pltpu.VMEM((128, 1024), bf16),
            pltpu.VMEM((8, 128), i32),
            pltpu.SemaphoreType.DMA((3,)),
        ],
        out_specs=[HBM] * 3,
    )(got, rows_t, base, r, ids, low, high, y_low, y_high, pairs, pair_hot, state, pos, vel, mass)
    return (read.reshape(19, WX, WY, WZ), vel_next, pos_next)


def solution(mesh):
    return jax.shard_map(
        local,
        mesh=mesh,
        in_specs=(
            P(None, "gx", "yz", None),
            P("gx", "yz", None),
            P(("gx", "yz"), None),
            P(None, ("gx", "yz")),
            P(None, ("gx", "yz")),
            P(None, ("gx", "yz")),
            P(("gx", "yz")),
            P(("gx", "yz")),
        ),
        out_specs=(P(None, "gx", "yz", None), P(None, ("gx", "yz")), P(None, ("gx", "yz"))),
        check_vma=False,
    )
```

```python
import jax
import jax.numpy as jnp
from jax import lax
from jax.experimental import pallas as pl
from jax.experimental.pallas import tpu as pltpu
from jax.sharding import PartitionSpec as P


lattice_dirs = (
    (0, 0, 0),
    (1, 0, 0),
    (-1, 0, 0),
    (0, 1, 0),
    (0, -1, 0),
    (0, 0, 1),
    (0, 0, -1),
    (1, 1, 0),
    (-1, -1, 0),
    (1, -1, 0),
    (-1, 1, 0),
    (1, 0, 1),
    (-1, 0, -1),
    (1, 0, -1),
    (-1, 0, 1),
    (0, 1, 1),
    (0, -1, -1),
    (0, 1, -1),
    (0, -1, 1),
)
lattice_weights = (1.0 / 3.0,) + (1.0 / 18.0,) * 6 + (1.0 / 36.0,) * 12
opposite = (0, 2, 1, 4, 3, 6, 5, 8, 7, 10, 9, 12, 11, 14, 13, 16, 15, 18, 17)
relax_rate = 1.25
stiffness = 0.5
damping = 0.5

from_low_x = (1, 7, 9, 11, 13)
from_high_x = (2, 8, 10, 12, 14)
from_low_y = (3, 7, 10, 15, 17)
from_high_y = (4, 9, 8, 18, 16)

fields = ((1, 0, 0), (0, 1, 0), (0, 0, 1), (1, 1, 0), (1, -1, 0), (1, 0, 1), (1, 0, -1), (0, 1, 1), (0, 1, -1))


def field_of(direction):
    vector = lattice_dirs[direction]
    if vector in fields:
        return fields.index(vector), 1.0
    return fields.index(tuple(-c for c in vector)), -1.0


WX, WY, WZ = 8, 8, 128
ROWS = WX * WY
VMEM = pl.BlockSpec(memory_space=pltpu.VMEM)
HBM = pl.BlockSpec(memory_space=pltpu.HBM)
f32 = jnp.float32
i32 = jnp.int32


def call(kernel, outs, scratch=(), limit=24, flops=1_000_000, in_specs=None, out_specs=None, aliases=None):
    def run(*args):
        return pl.pallas_call(
            kernel,
            out_shape=[jax.ShapeDtypeStruct(s, d) for s, d in outs],
            in_specs=in_specs or [VMEM] * len(args),
            out_specs=out_specs or [VMEM] * len(outs),
            scratch_shapes=list(scratch),
            input_output_aliases=aliases or {},
            compiler_params=pltpu.CompilerParams(vmem_limit_bytes=limit << 20),
            cost_estimate=pl.CostEstimate(flops=flops, bytes_accessed=1 << 20, transcendentals=0),
        )(*args)

    return run


def lane_take(table, index):
    return jnp.take_along_axis(table, index, axis=1, mode="promise_in_bounds")


def spread(row):
    return jnp.broadcast_to(row, (8, 128))


def sublane_iota():
    return lax.broadcasted_iota(i32, (8, 128), 0)


def lane_iota():
    return lax.broadcasted_iota(i32, (8, 128), 1)


def collide(pops):
    density = pops[0]
    for direction in range(1, 19):
        density = density + pops[direction]
    inverse = 1.0 / density
    speeds = []
    for compo in range(3):
        moment = None
        for direction in range(1, 19):
            factor = lattice_dirs[direction][compo]
            if factor == 1:
                moment = pops[direction] if moment is None else moment + pops[direction]
            elif factor == -1:
                moment = moment - pops[direction]
        speeds.append(moment * inverse)
    square = speeds[0] * speeds[0] + speeds[1] * speeds[1] + speeds[2] * speeds[2]
    rest = 1.0 - 1.5 * square
    keep = 1.0 - relax_rate
    scaled = relax_rate * density
    post = [None] * 19
    post[0] = keep * pops[0] + (lattice_weights[0] * scaled) * rest
    scale = {w: w * scaled for w in (1.0 / 18.0, 1.0 / 36.0)}
    for direction in range(1, 19, 2):
        along = None
        for compo in range(3):
            factor = lattice_dirs[direction][compo]
            if factor == 1:
                along = speeds[compo] if along is None else along + speeds[compo]
            elif factor == -1:
                along = along - speeds[compo]
        weight = scale[lattice_weights[direction]]
        even = weight * (rest + 4.5 * along * along)
        odd = weight * (3.0 * along)
        post[direction] = keep * pops[direction] + even + odd
        post[direction + 1] = keep * pops[direction + 1] + even - odd
    total = post[0]
    for direction in range(1, 19):
        total = total + post[direction]
    return post, total


def first_kernel(
    pop_in, ids_in, near_in, pairs_in, pos_in, vel_in, rad_in, mass_in,
    pop, ids, pairs, pos, vel, rad, mass, g, r, x_up, x_down, y_up, y_down, ask_out,
    near, ask, sems,
):
    def copy(k, src, dst):
        started = pltpu.make_async_copy(src, dst, sems.at[k])
        started.start()
        return started

    asking = copy(0, near_in, near)
    cells = copy(1, ids_in, ids)
    planes = ((0, WX - 1), (1, 2), (3, 4), (5, 6))
    arriving = [
        [copy(2 + 2 * n + m, pop_in.at[:, x], pop.at[:, x]) for m, x in enumerate(chunk)]
        for n, chunk in enumerate(planes)
    ]
    others = [
        copy(10 + k, src, dst)
        for k, (src, dst) in enumerate(
            ((pairs_in, pairs), (pos_in, pos), (vel_in, vel), (rad_in, rad), (mass_in, mass))
        )
    ]
    asking.wait()
    lane = lane_iota()
    sub = sublane_iota()
    for tile in range(16):
        row = near[0:1, (tile // 2) * 128 : (tile // 2) * 128 + 128]
        index = (8 * (tile % 2) + sub) * 8 + (lane & 7)
        ask[tile * 8 : tile * 8 + 8, :] = lane_take(spread(row), index)
    sent = copy(15, ask, ask_out)
    cells.wait()
    for n, x in ((n, x) for n, chunk in enumerate(planes) for x in chunk):
        if x == planes[n][0]:
            for arrival in arriving[n]:
                arrival.wait()
        pops = [pop[c, x] for c in range(19)]
        cell = ids[x * 8 : x * 8 + 8, :]
        fluid = cell < 0
        post, total = collide(pops)
        post = [jnp.where(fluid, p, 0.0) for p in post]
        total = jnp.where(fluid, total, 0.0)
        for c in range(19):
            g[c * ROWS + x * 8 : c * ROWS + x * 8 + 8, :] = post[c]
        r[x * 8 : x * 8 + 8, :] = total
        for at, names, out in ((WX - 1, from_low_x, x_up), (0, from_high_x, x_down)):
            if x == at:
                for k, c in enumerate(names):
                    out[k * 8 : k * 8 + 8, :] = post[c]
                out[40:48, :] = total
                out[48:56, :] = cell.astype(f32)
    for y, names, out in ((WY - 1, from_low_y, y_up), (0, from_high_y, y_down)):
        for k, c in enumerate(names):
            out[k * 8 : k * 8 + 8, :] = g[pl.ds(c * ROWS + y, 8, stride=8), :]
        out[40:48, :] = r[pl.ds(y, 8, stride=8), :]
        out[48:56, :] = ids[pl.ds(y, 8, stride=8), :].astype(f32)
    for other in others:
        other.wait()
    sent.wait()


def corner_kernel(y_up, y_down, low, high, out_one, out_two, out_up, out_down):
    zero = jnp.zeros((2, 128), f32)
    for src, out, y, k_low, k_high in (
        (y_up, out_up, WY - 1, from_low_x.index(7), from_high_x.index(10)),
        (y_down, out_down, 0, from_low_x.index(9), from_high_x.index(8)),
    ):
        out[0:56, :] = src[...]
        for at, halo, k in ((56, low, k_low), (59, high, k_high)):
            out[at : at + 1, :] = halo[k * 8 + y : k * 8 + y + 1, :]
            out[at + 1 : at + 2, :] = halo[40 + y : 41 + y, :]
            out[at + 2 : at + 3, :] = halo[48 + y : 49 + y, :]
        out[62:64, :] = zero
    even = lax.rem(lax.axis_index("yz"), 2) == 0
    out_one[...] = jnp.where(even, out_up[...], out_down[...])
    out_two[...] = jnp.where(even, out_down[...], out_up[...])


def shift_y(value, c_y, row):
    sub = sublane_iota()
    if c_y == 1:
        return jnp.where(sub == 0, spread(row), pltpu.roll(value, 1, 0))
    return jnp.where(sub == WY - 1, spread(row), pltpu.roll(value, WY - 1, 0))


def shift_z(value, c_z):
    return value if c_z == 0 else pltpu.roll(value, c_z % WZ, 1)


combos = ((0, 0), (1, 0), (-1, 0), (0, 1), (0, -1), (1, 1), (-1, -1), (1, -1), (-1, 1))


class Totals:
    def __init__(self, start=None):
        self.acc = start or [None] * 9

    def add(self, k, value, sign):
        if self.acc[k] is None:
            self.acc[k] = value if sign == 1 else -value
        else:
            self.acc[k] = self.acc[k] + value if sign == 1 else self.acc[k] - value

    def link(self, direction, came, near_r):
        vector = lattice_dirs[direction]
        pull = (-6.0 * lattice_weights[direction]) * near_r
        for compo in range(3):
            if vector[compo] != 0:
                self.add(compo, came, vector[compo])
                self.add(3 + compo, pull, 1)
        for n, (p, q) in enumerate(((0, 1), (0, 2), (1, 2))):
            if vector[p] * vector[q] != 0:
                self.add(6 + n, pull, vector[p] * vector[q])


def source_plane(g, low, high, direction, at):
    if at == -1:
        k = from_low_x.index(direction)
        return low[k * 8 : k * 8 + 8, :]
    if at == WX:
        k = from_high_x.index(direction)
        return high[k * 8 : k * 8 + 8, :]
    return g[direction * ROWS + at * 8 : direction * ROWS + at * 8 + 8, :]


def density_plane(r, low, high, at):
    return low[40:48, :] if at == -1 else high[40:48, :] if at == WX else r[at * 8 : at * 8 + 8, :]


def spread_slots(part, row, pick, names=range(9)):
    tiles = [
        jnp.where(pick, spread(part[half * 72 + v * 8 + row : half * 72 + v * 8 + row + 1, :]), 0.0)
        for half in range(2)
        for v in names
    ]
    return jnp.concatenate(tiles, 0).astype(jnp.bfloat16)


def split_fields(part, acc):
    for v in range(9):
        if acc[v] is None:
            continue
        value = 2.0 * acc[v] if v < 3 else acc[v]
        head = value.astype(jnp.bfloat16).astype(f32)
        part[v * 8 : v * 8 + 8, :] = head
        part[72 + v * 8 : 80 + v * 8, :] = value - head


def contract(left, right):
    return lax.dot_general(left, right, (((1,), (1,)), ((), ())), preferred_element_type=f32)


def early_kernel(
    g, r, pop, ids, low, high, pairs, pos, vel, rad,
    base, sums, edge_hot, pair_hot, state,
    shifted, part, left, hot, pair,
):
    sub = sublane_iota()

    def shift(value, c_y, c_z):
        if c_y == 1:
            value = jnp.where(sub == 0, 0.0, pltpu.roll(value, 1, 0))
        elif c_y == -1:
            value = jnp.where(sub == WY - 1, 0.0, pltpu.roll(value, WY - 1, 0))
        return shift_z(value, c_z)

    for at in range(-1, WX + 1):
        plain = density_plane(r, low, high, at)
        for k, (c_y, c_z) in enumerate(combos):
            if 0 <= at < WX or c_y == 0 or c_z == 0:
                shifted[k * 80 + (at + 1) * 8 : k * 80 + (at + 1) * 8 + 8, :] = shift(plain, c_y, c_z)
    number = lax.broadcasted_iota(i32, (128, 128), 0)
    total = jnp.zeros((144, 128), f32)
    for x in range(WX):
        fluid = ids[x * 8 : x * 8 + 8, :] < 0
        base[x * 8 : x * 8 + 8, :] = jnp.where(fluid, g[x * 8 : x * 8 + 8, :], pop[x * 8 : x * 8 + 8, :])
        links = Totals()
        for direction in range(1, 19):
            c_x, c_y, c_z = lattice_dirs[direction]
            row = combos.index((c_y, c_z)) * 80 + (x - c_x + 1) * 8
            near_r = shifted[row : row + 8, :]
            came = shift(source_plane(g, low, high, direction, x - c_x), c_y, c_z)
            at = direction * ROWS + x * 8
            back = opposite[direction] * ROWS + x * 8
            open_link = jnp.where(near_r != 0.0, came, g[back : back + 8, :])
            base[at : at + 8, :] = jnp.where(fluid, open_link, pop[at : at + 8, :])
            links.link(direction, came, near_r)
        split_fields(part, links.acc)
        for y in range(WY):
            key = ids[x * 8 + y : x * 8 + y + 1, :]
            left[:, y * 128 : y * 128 + 128] = spread_slots(part, y, spread(key & 7) == sub)
            owner = jnp.broadcast_to(key >> 3, (128, 128))
            one_hot = jnp.where(owner == number, 1.0, 0.0).astype(jnp.bfloat16)
            hot[:, y * 128 : y * 128 + 128] = one_hot
            if y in (0, WY - 1):
                to = (0 if y == 0 else 1024) + x * 128
                edge_hot[:, to : to + 128] = one_hot
        total = total + contract(left[...], hot[...])
    sums[...] = total[0:72, :] + total[72:144, :]
    for k in range(8):
        key = pairs[0:1, k * 128 : k * 128 + 128]
        pair[k : k + 1, :] = key
        rest = jnp.broadcast_to(key & 127, (128, 128))
        pair_hot[:, k * 128 : k * 128 + 128] = jnp.where(rest == number, 1.0, 0.0).astype(jnp.bfloat16)
    first = pair[...]
    held = held_states(pos, vel, rad, first >> 7, first & 127)
    for c, value in enumerate(held):
        state[c * 8 : c * 8 + 8, :] = value


edge_fields = (0, 1, 2, 3, 4, 5, 6, 8)


def complete_side(low_side, ids, halo, edge_hot, base, part, left):
    sub = sublane_iota()
    y = jnp.where(low_side, 0, WY - 1)
    sign = jnp.where(low_side, 1.0, -1.0)
    fluid = ids[pl.ds(y, 8, stride=8), :] < 0
    links = Totals()
    for k, direction in enumerate(from_low_y):
        c_x, _, c_z = lattice_dirs[direction]
        came = halo[k * 8 : k * 8 + 8, :]
        near_r = halo[40:48, :]
        if c_x == 1:
            came = jnp.where(sub == 0, spread(halo[56:57, :]), pltpu.roll(came, 1, 0))
            near_r = jnp.where(sub == 0, spread(halo[57:58, :]), pltpu.roll(near_r, 1, 0))
        elif c_x == -1:
            came = jnp.where(sub == WX - 1, spread(halo[59:60, :]), pltpu.roll(came, WX - 1, 0))
            near_r = jnp.where(sub == WX - 1, spread(halo[60:61, :]), pltpu.roll(near_r, WX - 1, 0))
        came = shift_z(came, c_z)
        near_r = shift_z(near_r, c_z)
        at = pl.ds(jnp.where(low_side, direction, from_high_y[k]) * ROWS + y, 8, stride=8)
        base[at, :] = jnp.where(fluid & (near_r != 0.0), came, base[at, :])
        links.link(direction, came, near_r)
    for v in (1, 6, 8):
        links.acc[v] = sign * links.acc[v]
    split_fields(part, links.acc)
    for x in range(WX):
        key = ids[pl.ds(x * 8 + y, 1), :]
        left[:, x * 128 : x * 128 + 128] = spread_slots(part, x, spread(key & 7) == sub, edge_fields)
    hot = edge_hot[:, pl.ds(pl.multiple_of(jnp.where(low_side, 0, 1024), 1024), 1024)]
    total = contract(left[...], hot)
    total = total[0:64, :] + total[64:128, :]
    return jnp.concatenate([total[0:56, :], jnp.zeros((8, 128), f32), total[56:64, :]], 0)


def held_states(pos, vel, rad, chunk, index):
    state = []
    for ref, count in ((pos, 3), (vel, 3), (rad, 1)):
        for c in range(count):
            value = jnp.zeros((8, 128), f32)
            for k in range(4):
                table = spread(ref[c : c + 1, k * 128 : k * 128 + 128])
                value = jnp.where(chunk == k, lane_take(table, index), value)
            state.append(value)
    return state


def reply_kernel(
    got, pos, vel, rad, sums_in, ids, y_one, y_two, edge_hot, base_in, out, rows_t, base, y_low, y_high, part, left
):
    even = lax.rem(lax.axis_index("yz"), 2) == 0
    sums = sums_in[...] + complete_side(even, ids, y_two, edge_hot, base, part, left)
    y_low[...] = jnp.where(even, y_two[...], y_one[...])
    y_high[...] = jnp.where(even, y_one[...], y_two[...])
    rows = got[...].astype(f32).T[0:8, :].astype(i32)
    rows_t[...] = rows
    state = held_states(pos, vel, rad, rows >> 7, rows & 127)
    out[pl.ds(0, 128, stride=2), :] = jnp.concatenate(state + [sums], 0).T
    lane = lane_iota()
    side = {-1: (lane & -8) | ((lane - 1) & 7), 1: (lane & -8) | ((lane + 1) & 7)}

    def moved(value, d_x, d_y):
        if d_x != 0:
            value = pltpu.roll(value, 8 if d_x == -1 else 120, 1)
        return value if d_y == 0 else lane_take(value, side[d_y])

    speed = state[3:6]
    plus = speed[0] + speed[1]
    minus = speed[0] - speed[1]
    rest = []
    for d_x, d_y in ((-1, 0), (1, 0), (0, -1), (0, 1)):
        rest += [moved(value, d_x, d_y) for value in speed]
    for d_x, d_y, value in ((-1, -1, plus), (1, -1, minus), (-1, 1, minus), (1, 1, plus)):
        rest.append(moved(value, d_x, d_y))
    out[pl.ds(1, 128, stride=2), :] = jnp.concatenate(rest, 0).T


def half_kernel(sums_in, ids, y_one, edge_hot, base_in, base, sums, part, left):
    low_side = lax.rem(lax.axis_index("yz"), 2) == 1
    sums[...] = sums_in[...] + complete_side(low_side, ids, y_one, edge_hot, base, part, left)


def look_up(ref, starts, cell):
    owner = (cell >> 3) & 127
    slot = jnp.where(cell >= 0, cell & 7, 8)
    values = [jnp.zeros((8, 128), f32) for start in starts]
    for s in range(8):
        chosen = slot == s
        for n, start in enumerate(starts):
            taken = lane_take(spread(ref[start + s : start + s + 1, :]), owner)
            values[n] = jnp.where(chosen, taken, values[n])
    return values


def last_kernel(
    got, rows_t, base, r, ids, low, high, y_low, y_high, pairs, pair_hot, state, pos, vel, mass,
    read_out, vel_out, pos_out,
    read, vel_next, pos_next, table, around, moving, rim, left, hot, pair, sems,
):
    table[...] = got[pl.ds(0, 128, stride=2), :].T
    around[...] = got[pl.ds(1, 128, stride=2), :].T
    number = lax.broadcasted_iota(i32, (128, 128), 0)
    for s in range(8):
        key = rows_t[s : s + 1, :]
        below = jnp.broadcast_to(jnp.where(key >= 0, key & 127, -1), (128, 128))
        hot[:, s * 128 : s * 128 + 128] = jnp.where(below == number, 1.0, 0.0).astype(jnp.bfloat16)

    def combine(values, vector):
        total = None
        for value, factor in zip(values, vector):
            if factor == 1:
                total = value if total is None else total + value
            elif factor == -1:
                total = total - value
        return total

    for x in range(WX):
        speeds = look_up(table, (24, 32, 40), ids[x * 8 : x * 8 + 8, :])
        for n, vector in enumerate(fields):
            moving[n * 80 + (x + 1) * 8 : n * 80 + (x + 1) * 8 + 8, :] = combine(speeds, vector)
    for at, halo, start in ((-1, low, 0), (WX, high, 24)):
        speeds = look_up(around, (start, start + 8, start + 16), halo[48:56, :].astype(i32))
        for n, vector in enumerate(fields):
            if vector[0] != 0:
                moving[n * 80 + (at + 1) * 8 : n * 80 + (at + 1) * 8 + 8, :] = combine(speeds, vector)
    for side, halo, start in ((0, y_low, 48), (1, y_high, 72)):
        speeds = look_up(around, (start, start + 8, start + 16), halo[48:56, :].astype(i32))
        for n, vector in enumerate(fields):
            if vector[1] != 0:
                rim[side * 72 + n * 8 : side * 72 + n * 8 + 8, :] = combine(speeds, vector)
    for n, (halo, row) in enumerate(((y_low, 58), (y_low, 61), (y_high, 58), (y_high, 61))):
        pair[n : n + 1, :] = halo[row : row + 1, :].astype(i32)
    cell = pair[0:4, :]
    owner = (cell >> 3) & 127
    slot = jnp.where(cell >= 0, cell & 7, 8)
    value = jnp.zeros((4, 128), f32)
    for s in range(8):
        value = jnp.where(slot == s, lane_take(around[pl.ds(96 + s, 4, stride=8), :], owner), value)
    rim[144:148, :] = value

    for x in range(WX):
        mine = r[x * 8 : x * 8 + 8, :]
        read[x * 8 : x * 8 + 8, :] = base[x * 8 : x * 8 + 8, :]
        for direction in range(1, 19):
            c_x, c_y, c_z = lattice_dirs[direction]
            n, sign = field_of(direction)
            at = x - c_x
            value = moving[n * 80 + (at + 1) * 8 : n * 80 + (at + 1) * 8 + 8, :]
            if c_y != 0:
                side = 0 if c_y == 1 else 1
                row = 144 + side * 2 if at == -1 else 145 + side * 2 if at == WX else side * 72 + n * 8 + at
                value = shift_y(value, c_y, rim[row : row + 1, :])
            value = shift_z(value, c_z)
            to = direction * ROWS + x * 8
            read[to : to + 8, :] = base[to : to + 8, :] + ((sign * 6.0 * lattice_weights[direction]) * mine) * value

    sent = pltpu.make_async_copy(read, read_out, sems.at[0])
    sent.start()

    @pl.when(lax.axis_index("gx") >= 0)
    def _():
        grains(rows_t, pairs, pair_hot, state, pos, vel, mass, vel_next, pos_next, table, left, hot, pair)

    outs = [pltpu.make_async_copy(vel_next, vel_out, sems.at[1]), pltpu.make_async_copy(pos_next, pos_out, sems.at[2])]
    for out in outs:
        out.start()
    for out in outs:
        out.wait()
    sent.wait()


def grains(rows_t, pairs, pair_hot, state, pos, vel, mass, vel_next, pos_next, table, left, hot, pair):
    for k in range(8):
        pair[k : k + 1, :] = pairs[1:2, k * 128 : k * 128 + 128]
    second = pair[...]
    state_a = [state[c * 8 : c * 8 + 8, :] for c in range(7)]
    state_b = look_up(table, tuple(8 * c for c in range(7)), second)
    offset = [a - b for a, b in zip(state_a[0:3], state_b[0:3])]
    length = jnp.sqrt(offset[0] * offset[0] + offset[1] * offset[1] + offset[2] * offset[2])
    inverse = 1.0 / jnp.maximum(length, 1.0)
    normal = [o * inverse for o in offset]
    inter = jnp.maximum(state_a[6] + state_b[6] - length, 0.0)
    closing = None
    for a, b, n in zip(state_a[3:6], state_b[3:6], normal):
        closing = (a - b) * n if closing is None else closing + (a - b) * n
    size = stiffness * inter - damping * inter * closing
    push = [size * n for n in normal]

    sub = sublane_iota()

    def by_block(values, key):
        pick = spread(key >> 7) == (sub & 3)
        tiles = ([], [])
        for n in range(0, len(values), 2):
            value = spread(values[n])
            if n + 1 < len(values):
                value = jnp.where(sub < 4, value, spread(values[n + 1]))
            value = jnp.where(pick, value, 0.0)
            head = value.astype(jnp.bfloat16).astype(f32)
            tiles[0].append(head)
            tiles[1].append(value - head)
        return jnp.concatenate(tiles[0] + tiles[1], 0).astype(jnp.bfloat16)

    for s in range(8):
        columns = slice(s * 128, s * 128 + 128)
        key = rows_t[s : s + 1, :]
        left[0:80, columns] = by_block([table[56 + v * 8 + s : 57 + v * 8 + s, :] for v in range(9)], key)
        left[80:112, columns] = by_block([p[s : s + 1, :] for p in push], pairs[0:1, columns])
    fluid = contract(left[0:80, :], hot[...])
    fluid = fluid[0:40, :] + fluid[40:80, :]
    contact = contract(left[80:112, :], pair_hot[...])
    contact = contact[0:16, :] + contact[16:32, :]
    matrix = ((3, 6, 7), (6, 4, 8), (7, 8, 5))
    for k in range(4):
        columns = slice(k * 128, k * 128 + 128)
        speed = [vel[c : c + 1, columns] for c in range(3)]
        for c in range(3):
            force = fluid[c * 4 + k : c * 4 + k + 1, :]
            for q in range(3):
                row = matrix[c][q] * 4 + k
                force = force + fluid[row : row + 1, :] * speed[q]
            fresh = speed[c] + (force + contact[c * 4 + k : c * 4 + k + 1, :]) / mass[:, columns]
            vel_next[c : c + 1, columns] = fresh
            pos_next[c : c + 1, columns] = pos[c : c + 1, columns] + fresh


def ring(axis, value, up):
    count = lax.axis_size(axis)
    pairs = [(i, (i + 1) % count) if up else ((i + 1) % count, i) for i in range(count)]
    return lax.ppermute(value, axis, pairs)


def swap(axis, value, offset):
    count = lax.axis_size(axis)
    pairs = []
    for i in range(offset, count + offset, 2):
        pairs += [(i % count, (i + 1) % count), ((i + 1) % count, i % count)]
    return lax.ppermute(value, axis, pairs)


def exchange(value):
    return lax.all_to_all(value, ("gx", "yz"), split_axis=0, concat_axis=0, tiled=True)


def local(
    populations,
    cell_grain,
    near_rows,
    contact_pairs,
    grain_position,
    grain_velocity,
    grain_radius,
    grain_mass,
):
    pop = populations
    ids = cell_grain.reshape(ROWS, 128)
    rad = grain_radius.reshape(1, 512)
    mass = grain_mass.reshape(1, 512)
    return step(pop, ids, near_rows, contact_pairs, grain_position, grain_velocity, rad, mass)


def step(pop, ids, near_rows, contact_pairs, grain_position, grain_velocity, rad, mass):
    slab = ((56, 128), f32)
    full = ((19 * ROWS, 128), f32)
    cells = (ROWS, 128)
    vector = ((3, 512), f32)
    scalar = ((1, 512), f32)
    bf16 = jnp.bfloat16
    pop, ids, pairs, pos, vel, rad, mass, g, r, x_up, x_down, y_up, y_down, ask = call(
        first_kernel,
        [((19, WX, WY, WZ), f32), (cells, i32), ((2, 1024), i32), vector, vector, scalar, scalar]
        + [full, (cells, f32), slab, slab, slab, slab, ((128, 128), i32)],
        [pltpu.VMEM((1, 1024), i32), pltpu.VMEM((128, 128), i32), pltpu.SemaphoreType.DMA((16,))],
        in_specs=[HBM] * 8,
        out_specs=[VMEM] * 13 + [HBM],
    )(
        *[
            pltpu.with_memory_space_constraint(value, pltpu.HBM)
            for value in (pop, ids, near_rows, contact_pairs, grain_position, grain_velocity, rad, mass)
        ]
    )
    pop = pop.reshape(19 * ROWS, 128)
    low = ring("gx", x_up, True)
    high = ring("gx", x_down, False)
    asked = exchange(ask)
    y_one, y_two = call(
        corner_kernel, [((64, 128), f32), ((64, 128), f32)], [pltpu.VMEM((64, 128), f32)] * 2
    )(y_up, y_down, low, high)
    y_one = swap("yz", y_one, 0)
    y_two = swap("yz", y_two, 1)
    base, sums, edge_hot, pair_hot, state = call(
        early_kernel,
        [full, ((72, 128), f32), ((128, 2048), bf16), ((128, 1024), bf16), ((56, 128), f32)],
        [
            pltpu.VMEM((9 * 80, 128), f32),
            pltpu.VMEM((144, 128), f32),
            pltpu.VMEM((144, 1024), bf16),
            pltpu.VMEM((128, 1024), bf16),
            pltpu.VMEM((8, 128), i32),
        ],
    )(g, r, pop, ids, low, high, pairs, pos, vel, rad)
    tail = [pltpu.VMEM((144, 128), f32), pltpu.VMEM((128, 1024), bf16)]
    base, sums = call(half_kernel, [full, ((72, 128), f32)], tail, aliases={4: 0})(
        sums, ids, y_one, edge_hot, base
    )
    send, rows_t, base, y_low, y_high = call(
        reply_kernel,
        [((256, 128), f32), ((8, 128), i32), full, ((64, 128), f32), ((64, 128), f32)],
        tail,
        aliases={9: 2},
    )(asked, pos, vel, rad, sums, ids, y_one, y_two, edge_hot, base)
    got = exchange(send.reshape(128, 2, 128)).reshape(256, 128)
    read, vel_next, pos_next = call(
        last_kernel,
        [full, vector, vector],
        [
            pltpu.VMEM((19 * ROWS, 128), f32),
            pltpu.VMEM((3, 512), f32),
            pltpu.VMEM((3, 512), f32),
            pltpu.VMEM((128, 128), f32),
            pltpu.VMEM((128, 128), f32),
            pltpu.VMEM((9 * 80, 128), f32),
            pltpu.VMEM((152, 128), f32),
            pltpu.VMEM((112, 1024), bf16),
            pltpu.VMEM((128, 1024), bf16),
            pltpu.VMEM((8, 128), i32),
            pltpu.SemaphoreType.DMA((3,)),
        ],
        out_specs=[HBM] * 3,
    )(got, rows_t, base, r, ids, low, high, y_low, y_high, pairs, pair_hot, state, pos, vel, mass)
    return (read.reshape(19, WX, WY, WZ), vel_next, pos_next)


def solution(mesh):
    return jax.shard_map(
        local,
        mesh=mesh,
        in_specs=(
            P(None, "gx", "yz", None),
            P("gx", "yz", None),
            P(("gx", "yz"), None),
            P(None, ("gx", "yz")),
            P(None, ("gx", "yz")),
            P(None, ("gx", "yz")),
            P(("gx", "yz")),
            P(("gx", "yz")),
        ),
        out_specs=(P(None, "gx", "yz", None), P(None, ("gx", "yz")), P(None, ("gx", "yz"))),
        check_vma=False,
    )
```

```python
import jax
import jax.numpy as jnp
from jax import lax
from jax.experimental import pallas as pl
from jax.experimental.pallas import tpu as pltpu
from jax.sharding import PartitionSpec as P


lattice_dirs = (
    (0, 0, 0),
    (1, 0, 0),
    (-1, 0, 0),
    (0, 1, 0),
    (0, -1, 0),
    (0, 0, 1),
    (0, 0, -1),
    (1, 1, 0),
    (-1, -1, 0),
    (1, -1, 0),
    (-1, 1, 0),
    (1, 0, 1),
    (-1, 0, -1),
    (1, 0, -1),
    (-1, 0, 1),
    (0, 1, 1),
    (0, -1, -1),
    (0, 1, -1),
    (0, -1, 1),
)
lattice_weights = (1.0 / 3.0,) + (1.0 / 18.0,) * 6 + (1.0 / 36.0,) * 12
opposite = (0, 2, 1, 4, 3, 6, 5, 8, 7, 10, 9, 12, 11, 14, 13, 16, 15, 18, 17)
relax_rate = 1.25
stiffness = 0.5
damping = 0.5

from_low_x = (1, 7, 9, 11, 13)
from_high_x = (2, 8, 10, 12, 14)
from_low_y = (3, 7, 10, 15, 17)
from_high_y = (4, 9, 8, 18, 16)

fields = ((1, 0, 0), (0, 1, 0), (0, 0, 1), (1, 1, 0), (1, -1, 0), (1, 0, 1), (1, 0, -1), (0, 1, 1), (0, 1, -1))


def field_of(direction):
    vector = lattice_dirs[direction]
    if vector in fields:
        return fields.index(vector), 1.0
    return fields.index(tuple(-c for c in vector)), -1.0


WX, WY, WZ = 8, 8, 128
ROWS = WX * WY
VMEM = pl.BlockSpec(memory_space=pltpu.VMEM)
HBM = pl.BlockSpec(memory_space=pltpu.HBM)
f32 = jnp.float32
i32 = jnp.int32


def call(kernel, outs, scratch=(), limit=24, flops=1_000_000, in_specs=None, out_specs=None, aliases=None):
    def run(*args):
        return pl.pallas_call(
            kernel,
            out_shape=[jax.ShapeDtypeStruct(s, d) for s, d in outs],
            in_specs=in_specs or [VMEM] * len(args),
            out_specs=out_specs or [VMEM] * len(outs),
            scratch_shapes=list(scratch),
            input_output_aliases=aliases or {},
            compiler_params=pltpu.CompilerParams(vmem_limit_bytes=limit << 20),
            cost_estimate=pl.CostEstimate(flops=flops, bytes_accessed=1 << 20, transcendentals=0),
        )(*args)

    return run


def lane_take(table, index):
    return jnp.take_along_axis(table, index, axis=1, mode="promise_in_bounds")


def spread(row):
    return jnp.broadcast_to(row, (8, 128))


def sublane_iota():
    return lax.broadcasted_iota(i32, (8, 128), 0)


def lane_iota():
    return lax.broadcasted_iota(i32, (8, 128), 1)


def collide(pops):
    density = pops[0]
    for direction in range(1, 19):
        density = density + pops[direction]
    inverse = 1.0 / density
    speeds = []
    for compo in range(3):
        moment = None
        for direction in range(1, 19):
            factor = lattice_dirs[direction][compo]
            if factor == 1:
                moment = pops[direction] if moment is None else moment + pops[direction]
            elif factor == -1:
                moment = moment - pops[direction]
        speeds.append(moment * inverse)
    square = speeds[0] * speeds[0] + speeds[1] * speeds[1] + speeds[2] * speeds[2]
    rest = 1.0 - 1.5 * square
    keep = 1.0 - relax_rate
    scaled = relax_rate * density
    post = [None] * 19
    post[0] = keep * pops[0] + (lattice_weights[0] * scaled) * rest
    scale = {w: w * scaled for w in (1.0 / 18.0, 1.0 / 36.0)}
    for direction in range(1, 19, 2):
        along = None
        for compo in range(3):
            factor = lattice_dirs[direction][compo]
            if factor == 1:
                along = speeds[compo] if along is None else along + speeds[compo]
            elif factor == -1:
                along = along - speeds[compo]
        weight = scale[lattice_weights[direction]]
        even = weight * (rest + 4.5 * along * along)
        odd = weight * (3.0 * along)
        post[direction] = keep * pops[direction] + even + odd
        post[direction + 1] = keep * pops[direction + 1] + even - odd
    total = post[0]
    for direction in range(1, 19):
        total = total + post[direction]
    return post, total


def first_kernel(
    pop_in, ids_in, near_in, pairs_in, pos_in, vel_in, rad_in, mass_in,
    pop, ids, pairs, pos, vel, rad, mass, g, r, x_up, x_down, y_up, y_down, ask_out,
    near, ask, sems,
):
    def copy(k, src, dst):
        started = pltpu.make_async_copy(src, dst, sems.at[k])
        started.start()
        return started

    asking = copy(0, near_in, near)
    cells = copy(1, ids_in, ids)
    planes = ((0, WX - 1), (1, 2), (3, 4), (5, 6))
    arriving = [
        [copy(2 + 2 * n + m, pop_in.at[:, x], pop.at[:, x]) for m, x in enumerate(chunk)]
        for n, chunk in enumerate(planes)
    ]
    asking.wait()
    lane = lane_iota()
    sub = sublane_iota()
    for tile in range(16):
        row = near[0:1, (tile // 2) * 128 : (tile // 2) * 128 + 128]
        index = (8 * (tile % 2) + sub) * 8 + (lane & 7)
        ask[tile * 8 : tile * 8 + 8, :] = lane_take(spread(row), index)
    sent = copy(15, ask, ask_out)
    others = [
        copy(10 + k, src, dst)
        for k, (src, dst) in enumerate(
            ((pairs_in, pairs), (pos_in, pos), (vel_in, vel), (rad_in, rad), (mass_in, mass))
        )
    ]
    cells.wait()
    for n, x in ((n, x) for n, chunk in enumerate(planes) for x in chunk):
        if x == planes[n][0]:
            for arrival in arriving[n]:
                arrival.wait()
        pops = [pop[c, x] for c in range(19)]
        cell = ids[x * 8 : x * 8 + 8, :]
        fluid = cell < 0
        post, total = collide(pops)
        post = [jnp.where(fluid, p, 0.0) for p in post]
        total = jnp.where(fluid, total, 0.0)
        for c in range(19):
            g[c * ROWS + x * 8 : c * ROWS + x * 8 + 8, :] = post[c]
        r[x * 8 : x * 8 + 8, :] = total
        for at, names, out in ((WX - 1, from_low_x, x_up), (0, from_high_x, x_down)):
            if x == at:
                for k, c in enumerate(names):
                    out[k * 8 : k * 8 + 8, :] = post[c]
                out[40:48, :] = total
                out[48:56, :] = cell.astype(f32)
    for y, names, out in ((WY - 1, from_low_y, y_up), (0, from_high_y, y_down)):
        for k, c in enumerate(names):
            out[k * 8 : k * 8 + 8, :] = g[pl.ds(c * ROWS + y, 8, stride=8), :]
        out[40:48, :] = r[pl.ds(y, 8, stride=8), :]
        out[48:56, :] = ids[pl.ds(y, 8, stride=8), :].astype(f32)
    for other in others:
        other.wait()
    sent.wait()


def corner_kernel(y_up, y_down, low, high, out_one, out_two, out_up, out_down):
    zero = jnp.zeros((2, 128), f32)
    for src, out, y, k_low, k_high in (
        (y_up, out_up, WY - 1, from_low_x.index(7), from_high_x.index(10)),
        (y_down, out_down, 0, from_low_x.index(9), from_high_x.index(8)),
    ):
        out[0:56, :] = src[...]
        for at, halo, k in ((56, low, k_low), (59, high, k_high)):
            out[at : at + 1, :] = halo[k * 8 + y : k * 8 + y + 1, :]
            out[at + 1 : at + 2, :] = halo[40 + y : 41 + y, :]
            out[at + 2 : at + 3, :] = halo[48 + y : 49 + y, :]
        out[62:64, :] = zero
    even = lax.rem(lax.axis_index("yz"), 2) == 0
    out_one[...] = jnp.where(even, out_up[...], out_down[...])
    out_two[...] = jnp.where(even, out_down[...], out_up[...])


def shift_y(value, c_y, row):
    sub = sublane_iota()
    if c_y == 1:
        return jnp.where(sub == 0, spread(row), pltpu.roll(value, 1, 0))
    return jnp.where(sub == WY - 1, spread(row), pltpu.roll(value, WY - 1, 0))


def shift_z(value, c_z):
    return value if c_z == 0 else pltpu.roll(value, c_z % WZ, 1)


combos = ((0, 0), (1, 0), (-1, 0), (0, 1), (0, -1), (1, 1), (-1, -1), (1, -1), (-1, 1))


class Totals:
    def __init__(self, start=None):
        self.acc = start or [None] * 9

    def add(self, k, value, sign):
        if self.acc[k] is None:
            self.acc[k] = value if sign == 1 else -value
        else:
            self.acc[k] = self.acc[k] + value if sign == 1 else self.acc[k] - value

    def link(self, direction, came, near_r):
        vector = lattice_dirs[direction]
        pull = (-6.0 * lattice_weights[direction]) * near_r
        for compo in range(3):
            if vector[compo] != 0:
                self.add(compo, came, vector[compo])
                self.add(3 + compo, pull, 1)
        for n, (p, q) in enumerate(((0, 1), (0, 2), (1, 2))):
            if vector[p] * vector[q] != 0:
                self.add(6 + n, pull, vector[p] * vector[q])


def source_plane(g, low, high, direction, at):
    if at == -1:
        k = from_low_x.index(direction)
        return low[k * 8 : k * 8 + 8, :]
    if at == WX:
        k = from_high_x.index(direction)
        return high[k * 8 : k * 8 + 8, :]
    return g[direction * ROWS + at * 8 : direction * ROWS + at * 8 + 8, :]


def density_plane(r, low, high, at):
    return low[40:48, :] if at == -1 else high[40:48, :] if at == WX else r[at * 8 : at * 8 + 8, :]


def spread_slots(part, row, pick, names=range(9)):
    tiles = [
        jnp.where(pick, spread(part[half * 72 + v * 8 + row : half * 72 + v * 8 + row + 1, :]), 0.0)
        for half in range(2)
        for v in names
    ]
    return jnp.concatenate(tiles, 0).astype(jnp.bfloat16)


def split_fields(part, acc):
    for v in range(9):
        if acc[v] is None:
            continue
        value = 2.0 * acc[v] if v < 3 else acc[v]
        head = value.astype(jnp.bfloat16).astype(f32)
        part[v * 8 : v * 8 + 8, :] = head
        part[72 + v * 8 : 80 + v * 8, :] = value - head


def contract(left, right):
    return lax.dot_general(left, right, (((1,), (1,)), ((), ())), preferred_element_type=f32)


def early_kernel(
    g, r, pop, ids, low, high, pairs, pos, vel, rad,
    base, sums, edge_hot, pair_hot, state,
    shifted, part, left, hot, pair,
):
    sub = sublane_iota()

    def shift(value, c_y, c_z):
        if c_y == 1:
            value = jnp.where(sub == 0, 0.0, pltpu.roll(value, 1, 0))
        elif c_y == -1:
            value = jnp.where(sub == WY - 1, 0.0, pltpu.roll(value, WY - 1, 0))
        return shift_z(value, c_z)

    for at in range(-1, WX + 1):
        plain = density_plane(r, low, high, at)
        for k, (c_y, c_z) in enumerate(combos):
            if 0 <= at < WX or c_y == 0 or c_z == 0:
                shifted[k * 80 + (at + 1) * 8 : k * 80 + (at + 1) * 8 + 8, :] = shift(plain, c_y, c_z)
    number = lax.broadcasted_iota(i32, (128, 128), 0)
    total = jnp.zeros((144, 128), f32)
    for x in range(WX):
        fluid = ids[x * 8 : x * 8 + 8, :] < 0
        base[x * 8 : x * 8 + 8, :] = jnp.where(fluid, g[x * 8 : x * 8 + 8, :], pop[x * 8 : x * 8 + 8, :])
        links = Totals()
        for direction in range(1, 19):
            c_x, c_y, c_z = lattice_dirs[direction]
            row = combos.index((c_y, c_z)) * 80 + (x - c_x + 1) * 8
            near_r = shifted[row : row + 8, :]
            came = shift(source_plane(g, low, high, direction, x - c_x), c_y, c_z)
            at = direction * ROWS + x * 8
            back = opposite[direction] * ROWS + x * 8
            open_link = jnp.where(near_r != 0.0, came, g[back : back + 8, :])
            base[at : at + 8, :] = jnp.where(fluid, open_link, pop[at : at + 8, :])
            links.link(direction, came, near_r)
        split_fields(part, links.acc)
        for y in range(WY):
            key = ids[x * 8 + y : x * 8 + y + 1, :]
            left[:, y * 128 : y * 128 + 128] = spread_slots(part, y, spread(key & 7) == sub)
            owner = jnp.broadcast_to(key >> 3, (128, 128))
            one_hot = jnp.where(owner == number, 1.0, 0.0).astype(jnp.bfloat16)
            hot[:, y * 128 : y * 128 + 128] = one_hot
            if y in (0, WY - 1):
                to = (0 if y == 0 else 1024) + x * 128
                edge_hot[:, to : to + 128] = one_hot
        total = total + contract(left[...], hot[...])
    sums[...] = total[0:72, :] + total[72:144, :]
    for k in range(8):
        key = pairs[0:1, k * 128 : k * 128 + 128]
        pair[k : k + 1, :] = key
        rest = jnp.broadcast_to(key & 127, (128, 128))
        pair_hot[:, k * 128 : k * 128 + 128] = jnp.where(rest == number, 1.0, 0.0).astype(jnp.bfloat16)
    first = pair[...]
    held = held_states(pos, vel, rad, first >> 7, first & 127)
    for c, value in enumerate(held):
        state[c * 8 : c * 8 + 8, :] = value


edge_fields = (0, 1, 2, 3, 4, 5, 6, 8)


def complete_side(low_side, ids, halo, edge_hot, base, part, left):
    sub = sublane_iota()
    y = jnp.where(low_side, 0, WY - 1)
    sign = jnp.where(low_side, 1.0, -1.0)
    fluid = ids[pl.ds(y, 8, stride=8), :] < 0
    links = Totals()
    for k, direction in enumerate(from_low_y):
        c_x, _, c_z = lattice_dirs[direction]
        came = halo[k * 8 : k * 8 + 8, :]
        near_r = halo[40:48, :]
        if c_x == 1:
            came = jnp.where(sub == 0, spread(halo[56:57, :]), pltpu.roll(came, 1, 0))
            near_r = jnp.where(sub == 0, spread(halo[57:58, :]), pltpu.roll(near_r, 1, 0))
        elif c_x == -1:
            came = jnp.where(sub == WX - 1, spread(halo[59:60, :]), pltpu.roll(came, WX - 1, 0))
            near_r = jnp.where(sub == WX - 1, spread(halo[60:61, :]), pltpu.roll(near_r, WX - 1, 0))
        came = shift_z(came, c_z)
        near_r = shift_z(near_r, c_z)
        at = pl.ds(jnp.where(low_side, direction, from_high_y[k]) * ROWS + y, 8, stride=8)
        base[at, :] = jnp.where(fluid & (near_r != 0.0), came, base[at, :])
        links.link(direction, came, near_r)
    for v in (1, 6, 8):
        links.acc[v] = sign * links.acc[v]
    split_fields(part, links.acc)
    for x in range(WX):
        key = ids[pl.ds(x * 8 + y, 1), :]
        left[:, x * 128 : x * 128 + 128] = spread_slots(part, x, spread(key & 7) == sub, edge_fields)
    hot = edge_hot[:, pl.ds(pl.multiple_of(jnp.where(low_side, 0, 1024), 1024), 1024)]
    total = contract(left[...], hot)
    total = total[0:64, :] + total[64:128, :]
    return jnp.concatenate([total[0:56, :], jnp.zeros((8, 128), f32), total[56:64, :]], 0)


def held_states(pos, vel, rad, chunk, index):
    state = []
    for ref, count in ((pos, 3), (vel, 3), (rad, 1)):
        for c in range(count):
            value = jnp.zeros((8, 128), f32)
            for k in range(4):
                table = spread(ref[c : c + 1, k * 128 : k * 128 + 128])
                value = jnp.where(chunk == k, lane_take(table, index), value)
            state.append(value)
    return state


def reply_kernel(
    got, pos, vel, rad, sums_in, ids, y_one, y_two, edge_hot, base_in, out, rows_t, hot, base, y_low, y_high, part, left
):
    even = lax.rem(lax.axis_index("yz"), 2) == 0
    sums = sums_in[...] + complete_side(even, ids, y_two, edge_hot, base, part, left)
    y_low[...] = jnp.where(even, y_two[...], y_one[...])
    y_high[...] = jnp.where(even, y_one[...], y_two[...])
    rows = got[...].astype(f32).T[0:8, :].astype(i32)
    rows_t[...] = rows
    state = held_states(pos, vel, rad, rows >> 7, rows & 127)
    out[pl.ds(0, 128, stride=2), :] = jnp.concatenate(state + [sums], 0).T
    lane = lane_iota()
    side = {-1: (lane & -8) | ((lane - 1) & 7), 1: (lane & -8) | ((lane + 1) & 7)}

    def moved(value, d_x, d_y):
        if d_x != 0:
            value = pltpu.roll(value, 8 if d_x == -1 else 120, 1)
        return value if d_y == 0 else lane_take(value, side[d_y])

    speed = state[3:6]
    plus = speed[0] + speed[1]
    minus = speed[0] - speed[1]
    rest = []
    for d_x, d_y in ((-1, 0), (1, 0), (0, -1), (0, 1)):
        rest += [moved(value, d_x, d_y) for value in speed]
    for d_x, d_y, value in ((-1, -1, plus), (1, -1, minus), (-1, 1, minus), (1, 1, plus)):
        rest.append(moved(value, d_x, d_y))
    out[pl.ds(1, 128, stride=2), :] = jnp.concatenate(rest, 0).T
    number = lax.broadcasted_iota(i32, (128, 128), 0)
    for s in range(8):
        key = rows[s : s + 1, :]
        below = jnp.broadcast_to(jnp.where(key >= 0, key & 127, -1), (128, 128))
        hot[:, s * 128 : s * 128 + 128] = jnp.where(below == number, 1.0, 0.0).astype(jnp.bfloat16)


def half_kernel(sums_in, ids, y_one, edge_hot, base_in, base, sums, part, left):
    low_side = lax.rem(lax.axis_index("yz"), 2) == 1
    sums[...] = sums_in[...] + complete_side(low_side, ids, y_one, edge_hot, base, part, left)


def look_up(ref, starts, cell):
    owner = (cell >> 3) & 127
    slot = jnp.where(cell >= 0, cell & 7, 8)
    values = [jnp.zeros((8, 128), f32) for start in starts]
    for s in range(8):
        chosen = slot == s
        for n, start in enumerate(starts):
            taken = lane_take(spread(ref[start + s : start + s + 1, :]), owner)
            values[n] = jnp.where(chosen, taken, values[n])
    return values


def last_kernel(
    got, rows_t, hot, base, r, ids, low, high, y_low, y_high, pairs, pair_hot, state, pos, vel, mass,
    read_out, vel_out, pos_out,
    read, vel_next, pos_next, table, around, moving, rim, left, pair, sems,
):
    table[...] = got[pl.ds(0, 128, stride=2), :].T
    around[...] = got[pl.ds(1, 128, stride=2), :].T

    def combine(values, vector):
        total = None
        for value, factor in zip(values, vector):
            if factor == 1:
                total = value if total is None else total + value
            elif factor == -1:
                total = total - value
        return total

    for x in range(WX):
        speeds = look_up(table, (24, 32, 40), ids[x * 8 : x * 8 + 8, :])
        for n, vector in enumerate(fields):
            moving[n * 80 + (x + 1) * 8 : n * 80 + (x + 1) * 8 + 8, :] = combine(speeds, vector)
    for at, halo, start in ((-1, low, 0), (WX, high, 24)):
        speeds = look_up(around, (start, start + 8, start + 16), halo[48:56, :].astype(i32))
        for n, vector in enumerate(fields):
            if vector[0] != 0:
                moving[n * 80 + (at + 1) * 8 : n * 80 + (at + 1) * 8 + 8, :] = combine(speeds, vector)
    for side, halo, start in ((0, y_low, 48), (1, y_high, 72)):
        speeds = look_up(around, (start, start + 8, start + 16), halo[48:56, :].astype(i32))
        for n, vector in enumerate(fields):
            if vector[1] != 0:
                rim[side * 72 + n * 8 : side * 72 + n * 8 + 8, :] = combine(speeds, vector)
    for n, (halo, row) in enumerate(((y_low, 58), (y_low, 61), (y_high, 58), (y_high, 61))):
        pair[n : n + 1, :] = halo[row : row + 1, :].astype(i32)
    cell = pair[0:4, :]
    owner = (cell >> 3) & 127
    slot = jnp.where(cell >= 0, cell & 7, 8)
    value = jnp.zeros((4, 128), f32)
    for s in range(8):
        value = jnp.where(slot == s, lane_take(around[pl.ds(96 + s, 4, stride=8), :], owner), value)
    rim[144:148, :] = value

    for x in range(WX):
        mine = r[x * 8 : x * 8 + 8, :]
        read[x * 8 : x * 8 + 8, :] = base[x * 8 : x * 8 + 8, :]
        for direction in range(1, 19):
            c_x, c_y, c_z = lattice_dirs[direction]
            n, sign = field_of(direction)
            at = x - c_x
            value = moving[n * 80 + (at + 1) * 8 : n * 80 + (at + 1) * 8 + 8, :]
            if c_y != 0:
                side = 0 if c_y == 1 else 1
                row = 144 + side * 2 if at == -1 else 145 + side * 2 if at == WX else side * 72 + n * 8 + at
                value = shift_y(value, c_y, rim[row : row + 1, :])
            value = shift_z(value, c_z)
            to = direction * ROWS + x * 8
            read[to : to + 8, :] = base[to : to + 8, :] + ((sign * 6.0 * lattice_weights[direction]) * mine) * value

    sent = pltpu.make_async_copy(read, read_out, sems.at[0])
    sent.start()

    @pl.when(lax.axis_index("gx") >= 0)
    def _():
        grains(rows_t, pairs, pair_hot, state, pos, vel, mass, vel_next, pos_next, table, left, hot, pair)

    outs = [pltpu.make_async_copy(vel_next, vel_out, sems.at[1]), pltpu.make_async_copy(pos_next, pos_out, sems.at[2])]
    for out in outs:
        out.start()
    for out in outs:
        out.wait()
    sent.wait()


def grains(rows_t, pairs, pair_hot, state, pos, vel, mass, vel_next, pos_next, table, left, hot, pair):
    for k in range(8):
        pair[k : k + 1, :] = pairs[1:2, k * 128 : k * 128 + 128]
    second = pair[...]
    state_a = [state[c * 8 : c * 8 + 8, :] for c in range(7)]
    state_b = look_up(table, tuple(8 * c for c in range(7)), second)
    offset = [a - b for a, b in zip(state_a[0:3], state_b[0:3])]
    length = jnp.sqrt(offset[0] * offset[0] + offset[1] * offset[1] + offset[2] * offset[2])
    inverse = 1.0 / jnp.maximum(length, 1.0)
    normal = [o * inverse for o in offset]
    inter = jnp.maximum(state_a[6] + state_b[6] - length, 0.0)
    closing = None
    for a, b, n in zip(state_a[3:6], state_b[3:6], normal):
        closing = (a - b) * n if closing is None else closing + (a - b) * n
    size = stiffness * inter - damping * inter * closing
    push = [size * n for n in normal]

    sub = sublane_iota()

    def by_block(values, key):
        pick = spread(key >> 7) == (sub & 3)
        tiles = ([], [])
        for n in range(0, len(values), 2):
            value = spread(values[n])
            if n + 1 < len(values):
                value = jnp.where(sub < 4, value, spread(values[n + 1]))
            value = jnp.where(pick, value, 0.0)
            head = value.astype(jnp.bfloat16).astype(f32)
            tiles[0].append(head)
            tiles[1].append(value - head)
        return jnp.concatenate(tiles[0] + tiles[1], 0).astype(jnp.bfloat16)

    for s in range(8):
        columns = slice(s * 128, s * 128 + 128)
        key = rows_t[s : s + 1, :]
        left[0:80, columns] = by_block([table[56 + v * 8 + s : 57 + v * 8 + s, :] for v in range(9)], key)
        left[80:112, columns] = by_block([p[s : s + 1, :] for p in push], pairs[0:1, columns])
    fluid = contract(left[0:80, :], hot[...])
    fluid = fluid[0:40, :] + fluid[40:80, :]
    contact = contract(left[80:112, :], pair_hot[...])
    contact = contact[0:16, :] + contact[16:32, :]
    matrix = ((3, 6, 7), (6, 4, 8), (7, 8, 5))
    for k in range(4):
        columns = slice(k * 128, k * 128 + 128)
        speed = [vel[c : c + 1, columns] for c in range(3)]
        for c in range(3):
            force = fluid[c * 4 + k : c * 4 + k + 1, :]
            for q in range(3):
                row = matrix[c][q] * 4 + k
                force = force + fluid[row : row + 1, :] * speed[q]
            fresh = speed[c] + (force + contact[c * 4 + k : c * 4 + k + 1, :]) / mass[:, columns]
            vel_next[c : c + 1, columns] = fresh
            pos_next[c : c + 1, columns] = pos[c : c + 1, columns] + fresh


def ring(axis, value, up):
    count = lax.axis_size(axis)
    pairs = [(i, (i + 1) % count) if up else ((i + 1) % count, i) for i in range(count)]
    return lax.ppermute(value, axis, pairs)


def swap(axis, value, offset):
    count = lax.axis_size(axis)
    pairs = []
    for i in range(offset, count + offset, 2):
        pairs += [(i % count, (i + 1) % count), ((i + 1) % count, i % count)]
    return lax.ppermute(value, axis, pairs)


def exchange(value):
    return lax.all_to_all(value, ("gx", "yz"), split_axis=0, concat_axis=0, tiled=True)


def local(
    populations,
    cell_grain,
    near_rows,
    contact_pairs,
    grain_position,
    grain_velocity,
    grain_radius,
    grain_mass,
):
    pop = populations
    ids = cell_grain.reshape(ROWS, 128)
    rad = grain_radius.reshape(1, 512)
    mass = grain_mass.reshape(1, 512)
    return step(pop, ids, near_rows, contact_pairs, grain_position, grain_velocity, rad, mass)


def step(pop, ids, near_rows, contact_pairs, grain_position, grain_velocity, rad, mass):
    slab = ((56, 128), f32)
    full = ((19 * ROWS, 128), f32)
    cells = (ROWS, 128)
    vector = ((3, 512), f32)
    scalar = ((1, 512), f32)
    bf16 = jnp.bfloat16
    pop, ids, pairs, pos, vel, rad, mass, g, r, x_up, x_down, y_up, y_down, ask = call(
        first_kernel,
        [((19, WX, WY, WZ), f32), (cells, i32), ((2, 1024), i32), vector, vector, scalar, scalar]
        + [full, (cells, f32), slab, slab, slab, slab, ((128, 128), i32)],
        [pltpu.VMEM((1, 1024), i32), pltpu.VMEM((128, 128), i32), pltpu.SemaphoreType.DMA((16,))],
        in_specs=[HBM] * 8,
        out_specs=[VMEM] * 13 + [HBM],
    )(
        *[
            pltpu.with_memory_space_constraint(value, pltpu.HBM)
            for value in (pop, ids, near_rows, contact_pairs, grain_position, grain_velocity, rad, mass)
        ]
    )
    pop = pop.reshape(19 * ROWS, 128)
    low = ring("gx", x_up, True)
    high = ring("gx", x_down, False)
    asked = exchange(ask)
    y_one, y_two = call(
        corner_kernel, [((64, 128), f32), ((64, 128), f32)], [pltpu.VMEM((64, 128), f32)] * 2
    )(y_up, y_down, low, high)
    y_one = swap("yz", y_one, 0)
    y_two = swap("yz", y_two, 1)
    base, sums, edge_hot, pair_hot, state = call(
        early_kernel,
        [full, ((72, 128), f32), ((128, 2048), bf16), ((128, 1024), bf16), ((56, 128), f32)],
        [
            pltpu.VMEM((9 * 80, 128), f32),
            pltpu.VMEM((144, 128), f32),
            pltpu.VMEM((144, 1024), bf16),
            pltpu.VMEM((128, 1024), bf16),
            pltpu.VMEM((8, 128), i32),
        ],
    )(g, r, pop, ids, low, high, pairs, pos, vel, rad)
    tail = [pltpu.VMEM((144, 128), f32), pltpu.VMEM((128, 1024), bf16)]
    base, sums = call(half_kernel, [full, ((72, 128), f32)], tail, aliases={4: 0})(
        sums, ids, y_one, edge_hot, base
    )
    send, rows_t, list_hot, base, y_low, y_high = call(
        reply_kernel,
        [((256, 128), f32), ((8, 128), i32), ((128, 1024), bf16), full, ((64, 128), f32), ((64, 128), f32)],
        tail,
        aliases={9: 3},
    )(asked, pos, vel, rad, sums, ids, y_one, y_two, edge_hot, base)
    got = exchange(send.reshape(128, 2, 128)).reshape(256, 128)
    read, vel_next, pos_next = call(
        last_kernel,
        [full, vector, vector],
        [
            pltpu.VMEM((19 * ROWS, 128), f32),
            pltpu.VMEM((3, 512), f32),
            pltpu.VMEM((3, 512), f32),
            pltpu.VMEM((128, 128), f32),
            pltpu.VMEM((128, 128), f32),
            pltpu.VMEM((9 * 80, 128), f32),
            pltpu.VMEM((152, 128), f32),
            pltpu.VMEM((112, 1024), bf16),
            pltpu.VMEM((8, 128), i32),
            pltpu.SemaphoreType.DMA((3,)),
        ],
        out_specs=[HBM] * 3,
    )(got, rows_t, list_hot, base, r, ids, low, high, y_low, y_high, pairs, pair_hot, state, pos, vel, mass)
    return (read.reshape(19, WX, WY, WZ), vel_next, pos_next)


def solution(mesh):
    return jax.shard_map(
        local,
        mesh=mesh,
        in_specs=(
            P(None, "gx", "yz", None),
            P("gx", "yz", None),
            P(("gx", "yz"), None),
            P(None, ("gx", "yz")),
            P(None, ("gx", "yz")),
            P(None, ("gx", "yz")),
            P(("gx", "yz")),
            P(("gx", "yz")),
        ),
        out_specs=(P(None, "gx", "yz", None), P(None, ("gx", "yz")), P(None, ("gx", "yz"))),
        check_vma=False,
    )
```
